256 devices in a mesh: fsdp: 32 (over y_lo, z, core), tp: 8 (over x, y_hi).
Axes of the slice: x: 4, y: 4 (y_hi: 2, y_lo: 2; y = y_hi * 2 + y_lo), z: 8, core: 2. Of those that a mesh axis runs over, the one named last changes fastest.
Arguments:
- hidden: bfloat16 [64, 5120], P(None, 'fsdp'), may hold values from -20 to 20
- query_weight: bfloat16 [5120, 5120], P(None, ('tp', 'fsdp')), may hold values from -0.078125 to 0.078125
- key_weight: bfloat16 [5120, 1024], P(None, ('tp', 'fsdp')), may hold values from -0.078125 to 0.078125
- value_weight: bfloat16 [5120, 1024], P(None, ('tp', 'fsdp')), may hold values from -0.078125 to 0.078125
- output_weight: bfloat16 [5120, 5120], P(('tp', 'fsdp')), may hold values from -0.078125 to 0.078125
- gate_weight: bfloat16 [5120, 27648], P(None, ('tp', 'fsdp')), may hold values from -0.078125 to 0.078125
- up_weight: bfloat16 [5120, 27648], P(None, ('tp', 'fsdp')), may hold values from -0.078125 to 0.078125
- down_weight: bfloat16 [27648, 5120], P(('tp', 'fsdp')), may hold values from -0.0390625 to 0.0390625
- history: float32 [7, 1024], replicated, may hold values from 0.0001 to 1, as said below
- slot: int32 [1], replicated, may hold values from 0 to 1023
- lengths: int32 [64], P('fsdp'), may hold values from 512 to 4096, as said below
- key_cache: bfloat16 [64, 4096, 1024], P('fsdp', None, 'tp'), may hold values from -1000 to 1000
- value_cache: bfloat16 [64, 4096, 1024], P('fsdp', None, 'tp'), may hold values from -6 to 6
Outputs:
- attention_out: bfloat16 [64, 5120], P('fsdp', 'tp')
- query_rollout: bfloat16 [5120, 5120], P('fsdp', 'tp')
- key_rollout: bfloat16 [5120, 1024], P('fsdp', 'tp')
- value_rollout: bfloat16 [5120, 1024], P('fsdp', 'tp')
- output_rollout: bfloat16 [5120, 5120], P('tp', 'fsdp')
- gate_rollout: bfloat16 [5120, 27648], P('fsdp', 'tp')
- up_rollout: bfloat16 [5120, 27648], P('fsdp', 'tp')
- down_rollout: bfloat16 [27648, 5120], P('tp', 'fsdp')
- new_history: float32 [7, 1024], replicated
The draws below stay inside these ranges and needn't reach their ends.
Inputs may be any that keep to these rules, and one draw needn't show every extreme that they name: `history`: strictly positive. `lengths`: some sequence has all 4096 slots valid.
All inputs are finite; a program needn't handle non-finite values.
Results may differ from the reference program's by a relative error of at most 0.012.
The reference program's roundings to bfloat16 on the way (of `probs`) count: a program that leaves them out, or rounds other values in their place, can miss the bound.
Values may be sent and summed in bfloat16 or wider, within the bound.
A program may use at most 64 MiB of HBM per device.

```python
import jax
import jax.numpy as jnp
from jax import lax

D = 5120
F = 27648
HEADS = 40
KV_HEADS = 8
HEAD_DIM = 128
HIST = 1024
CACHE = 4096
SEQS = 64


def draw_hidden(key, part):
    values = jnp.clip(jax.random.normal(jax.random.fold_in(key, 11), (SEQS, D), jnp.float32), -6.0, 6.0)
    return values.astype(jnp.bfloat16)


def draw_history(key, part):
    fans = jnp.array([D, D, D, D, D, D, F], jnp.float32)
    low, high = (3.0, 12.0)
    levels = jnp.exp(jax.random.uniform(jax.random.fold_in(key, 21), (7,), jnp.float32, jnp.log(low), jnp.log(high)))
    spread = jnp.exp(jax.random.uniform(jax.random.fold_in(key, 22), (7, HIST), jnp.float32, jnp.log(0.02), 0.0))
    return (fans ** (-0.5) * levels)[:, None] * spread


def draw_lengths(key, part):
    counts = jax.random.randint(jax.random.fold_in(key, 31), (SEQS,), CACHE // 8, CACHE + 1)
    chosen = jax.random.randint(jax.random.fold_in(key, 32), (), 0, SEQS)
    return jnp.where(jnp.arange(SEQS) == chosen, CACHE, counts).astype(jnp.int32)


def draw_key_cache(key, part):
    values = jnp.clip(jax.random.normal(jax.random.fold_in(key, 41), (SEQS, CACHE, KV_HEADS * HEAD_DIM), jnp.float32), -6.0, 6.0)
    return values.astype(jnp.bfloat16)


def block_scale(own_key, shape, cuts, low, top_value):
    level, own = 1.0, jax.random.fold_in(own_key, 6)
    for dim, shards_of in cuts:
        heights = jnp.exp(jax.random.uniform(jax.random.fold_in(own, dim), (shards_of,), jnp.float32, low / len(cuts), top_value / len(cuts)))
        level = level * jnp.repeat(heights, shape[dim] // shards_of).reshape([-1 if axis == dim else 1 for axis in range(len(shape))])
    return level


def scatter_about(rng, extent, width, reach, cuts=(), kind=jnp.bfloat16):
    loudness = block_scale(rng, extent, cuts, -0.22, 0.18) if cuts else 1.0
    values = jax.random.normal(rng, extent, jnp.float32) * width * loudness
    return jnp.minimum(jnp.maximum(values, -reach), reach).astype(kind)


def setup_inputs(seed: int = 0) -> dict:
    streams_of = jax.random.split(jax.random.key(seed), 14)
    hidden = draw_hidden(jax.random.fold_in(streams_of[13], 71), 0)
    query_weight = scatter_about(streams_of[1], (D, D), D ** -0.5, 0.078125, ((1, 256),))
    key_weight = scatter_about(streams_of[2], (D, KV_HEADS * HEAD_DIM), D ** -0.5, 0.078125, ((1, 256),))
    value_weight = scatter_about(streams_of[3], (D, KV_HEADS * HEAD_DIM), D ** -0.5, 0.078125, ((1, 256),))
    output_weight = scatter_about(streams_of[4], (D, D), D ** -0.5, 0.078125, ((0, 256),))
    gate_weight = scatter_about(streams_of[5], (D, F), D ** -0.5, 0.078125, ((1, 256),))
    up_weight = scatter_about(streams_of[6], (D, F), D ** -0.5, 0.078125, ((1, 256),))
    down_weight = scatter_about(streams_of[7], (F, D), F ** -0.5, 0.0390625, ((0, 256),))
    history = draw_history(jax.random.fold_in(streams_of[13], 71), 0)
    slot = jax.random.randint(streams_of[9], (1,), 0, HIST).astype(jnp.int32)
    lengths = draw_lengths(jax.random.fold_in(streams_of[13], 71), 0)
    key_cache = draw_key_cache(jax.random.fold_in(streams_of[13], 71), 0)
    value_cache = scatter_about(streams_of[12], (SEQS, CACHE, KV_HEADS * HEAD_DIM), 1.0, 6.0, ((0, 32), (2, 8)))
    return dict(hidden=hidden, query_weight=query_weight, key_weight=key_weight, value_weight=value_weight, output_weight=output_weight, gate_weight=gate_weight, up_weight=up_weight, down_weight=down_weight, history=history, slot=slot, lengths=lengths, key_cache=key_cache, value_cache=value_cache)


target_peak = 4.0
norm_eps = 1e-06
rope_theta = 1000000.0

def largest(tensor):
    return jnp.max(jnp.abs(tensor.astype(jnp.float32)))

def scaling(peaks, history, slot):
    marked = lax.broadcasted_iota(jnp.int32, history.shape, 1) == slot[0]
    kept = lax.optimization_barrier(jnp.max(jnp.where(marked, jnp.zeros_like(history), history), axis=1))
    return (target_peak / jnp.maximum(peaks, kept), jnp.where(marked, peaks[:, None], history))

def quantize(tensor, factor):
    return (tensor.astype(jnp.float32) * factor).astype(jnp.bfloat16)

def rotate(vectors, positions):
    half_dim = vectors.shape[-1] // 2
    ladder = jnp.arange(half_dim, dtype=jnp.float32)
    spread = rope_theta ** (-2.0 * ladder / vectors.shape[-1])
    angle = positions.astype(jnp.float32)[:, None] * spread[None, :]
    cosine = jnp.cos(angle)[:, None, :]
    sine = jnp.sin(angle)[:, None, :]
    first = vectors[..., :half_dim]
    second = vectors[..., half_dim:]
    return jnp.concatenate([first * cosine - second * sine, second * cosine + first * sine], axis=-1)

def one_sequence(items):
    query, key_new, value_new, cached_keys, cached_values, length = items
    kv_count = query.shape[0]
    head_dim = query.shape[2]
    cache_len = cached_keys.shape[0]
    keys = cached_keys.reshape(cache_len, kv_count, head_dim).astype(jnp.float32)
    values = cached_values.reshape(cache_len, kv_count, head_dim).astype(jnp.float32)
    scale = head_dim ** (-0.5)
    widened = query.astype(jnp.float32)
    scores = jnp.einsum('kgd,jkd->kgj', widened, keys) * scale
    own = lax.optimization_barrier(jnp.sum(widened * key_new.astype(jnp.float32)[:, None, :], axis=-1)) * scale
    valid = (lax.broadcasted_iota(jnp.int32, (cache_len,), 0) < length)[None, None, :]
    top = jnp.maximum(lax.optimization_barrier(jnp.max(jnp.where(valid, scores, -1e+30), axis=-1)), own)
    weights = jnp.where(valid, jnp.exp(scores - top[..., None]), 0.0)
    own_weight = jnp.exp(own - top)
    total = lax.optimization_barrier(jnp.sum(weights, axis=-1)) + own_weight
    probs = (weights / total[..., None]).astype(jnp.bfloat16)
    own_prob = (own_weight / total).astype(jnp.bfloat16)
    mixed = jnp.einsum('kgj,jkd->kgd', probs.astype(jnp.float32), values)
    mixed = mixed + own_prob.astype(jnp.float32)[..., None] * value_new.astype(jnp.float32)[:, None, :]
    return mixed.astype(jnp.bfloat16).reshape(-1)

def reference(hidden, query_weight, key_weight, value_weight, output_weight, gate_weight, up_weight, down_weight, history, slot, lengths, key_cache, value_cache):
    trainer = [query_weight, key_weight, value_weight, output_weight, gate_weight, up_weight, down_weight]
    peaks = jnp.stack([largest(tensor) for tensor in trainer])
    factors, new_history = scaling(peaks, history, slot)
    rollout = [quantize(trainer[number], factors[number]) for number in range(7)]
    widened = hidden.astype(jnp.float32)
    inv_rms = lax.rsqrt(lax.optimization_barrier(jnp.mean(widened * widened, axis=1)) + norm_eps)[:, None]
    query = jnp.dot(hidden, rollout[0], preferred_element_type=jnp.float32) * inv_rms / factors[0]
    key_new = jnp.dot(hidden, rollout[1], preferred_element_type=jnp.float32) * inv_rms / factors[1]
    value_new = jnp.dot(hidden, rollout[2], preferred_element_type=jnp.float32) * inv_rms / factors[2]
    count_seq = hidden.shape[0]
    query = rotate(query.reshape(count_seq, HEADS, HEAD_DIM), lengths).astype(jnp.bfloat16)
    query = query.reshape(count_seq, KV_HEADS, HEADS // KV_HEADS, HEAD_DIM)
    key_new = rotate(key_new.reshape(count_seq, KV_HEADS, HEAD_DIM), lengths).astype(jnp.bfloat16)
    value_new = value_new.reshape(count_seq, KV_HEADS, HEAD_DIM).astype(jnp.bfloat16)
    attention_out = lax.map(one_sequence, (query, key_new, value_new, key_cache, value_cache, lengths))
    return (attention_out, rollout[0], rollout[1], rollout[2], rollout[3], rollout[4], rollout[5], rollout[6], new_history)
```

```python
import functools
import math

import jax
import jax.numpy as jnp
import numpy as np
from jax import lax
from jax.experimental import pallas as pl
from jax.experimental.pallas import tpu as pltpu
from jax.sharding import PartitionSpec as P

D = 5120
HEADS = 40
KV_HEADS = 8
HEAD_DIM = 128
GROUP = HEADS // KV_HEADS
CACHE = 4096
HIST = 1024
N = 32
TP = 8
ROWS = D // N
WIDE = 27648 // (N * TP)
SLIM = D // (N * TP)
TINY = KV_HEADS * HEAD_DIM // (N * TP)
LANES = 128
HEAD_COLS = LANES - SLIM - 2 * TINY
REST = WIDE - HEAD_COLS
CHUNK = 512

target_peak = 4.0
norm_eps = 1e-06
rope_theta = 1000000.0

F32 = jnp.float32
BF16 = jnp.bfloat16
MESH = pl.DeviceIdType.MESH


def offset(i):
    k = i // 4
    return (i // 2) % 2, ((k + 1) // 2) * (2 * (k % 2) - 1), i % 2


def kernel(
    hid, wq_h, wk_h, wv_h, wo_h, wg_h, wu_h, wd_h, hist, slot, lens, kc_h, vc_h, spread,
    att_o, q_o, k_o, v_o, o_o, g_o, u_o, d_o, nh_o,
    wq, wk, wv, wo, wg, wu, wd, kc, vc, sent, got, fac,
    pk_s, pk_r, pt_s, pt_r, part, one_r, two_s, two_r,
    load_sem, send_sem, recv_sem, pks_sem, pkr_sem, pts_sem, ptr_sem,
    ones_sem, oner_sem, twos_sem, twor_sem,
):
    me = lax.axis_index("fsdp")
    tp = lax.axis_index("tp")
    my_y, my_z, my_c = me // 16, (me // 2) % 8, me % 2

    def target(i):
        dy, dz, dc = offset(i)
        return ((my_y + dy) % 2) * 16 + ((my_z + dz + 8) % 8) * 2 + (my_c + dc) % 2

    def source(i):
        dy, dz, dc = offset(i)
        return ((my_y + dy) % 2) * 16 + ((my_z - dz + 8) % 8) * 2 + (my_c + dc) % 2

    barrier = pltpu.get_barrier_semaphore()

    def greet(i, _):
        pl.semaphore_signal(barrier, 1, device_id={"fsdp": target(i)}, device_id_type=MESH)
        return 0

    lax.fori_loop(1, N, greet, 0)

    def greet_tp(i, _):
        pl.semaphore_signal(barrier, 1, device_id={"tp": (tp + i) % TP}, device_id_type=MESH)
        return 0

    lax.fori_loop(1, TP, greet_tp, 0)

    loads = [
        pltpu.make_async_copy(src, dst, load_sem.at[n])
        for n, (src, dst) in enumerate(
            [(wg_h, wg), (wq_h, wq), (wk_h, wk), (wv_h, wv), (wu_h, wu), (wd_h, wd), (wo_h, wo), (kc_h, kc), (vc_h, vc)]
        )
    ]
    for load in loads:
        load.start()

    shift = (WIDE * me) % LANES

    def pack(tile, parts):
        def body(c, _):
            cols = pl.ds(pl.multiple_of(c * CHUNK, CHUNK), CHUNK)
            pieces = [ref[lo:hi, cols].astype(F32) for ref, lo, hi in parts]
            rows = sum(hi - lo for _, lo, hi in parts)
            if rows < LANES:
                pieces.append(jnp.zeros((LANES - rows, CHUNK), F32))
            block = jnp.concatenate(pieces, axis=0).T
            sent[tile, cols, :] = pltpu.roll(block, shift, 1).astype(BF16)
            return 0

        lax.fori_loop(0, D // CHUNK, body, 0)

    def block_copy(tile, to, slot_of):
        return pltpu.make_async_remote_copy(
            sent.at[tile, pl.ds(pl.multiple_of(to * ROWS, ROWS), ROWS)],
            got.at[tile, slot_of],
            send_sem.at[tile, to],
            recv_sem.at[tile, slot_of],
            device_id={"fsdp": to},
            device_id_type=MESH,
        )

    def send(tile):
        def body(j, _):
            block_copy(tile, target(N - 1 - j), me).start()
            return 0

        lax.fori_loop(0, N - 1, body, 0)

    for n in range(4):
        loads[n].wait()
    pack(0, [(wg, 0, HEAD_COLS), (wq, 0, SLIM), (wk, 0, TINY), (wv, 0, TINY)])
    for n in range(4, 7):
        loads[n].wait()

    lane = lax.broadcasted_iota(jnp.int32, (1, LANES), 1)
    mine = jnp.zeros((1, LANES), F32)
    for t, ref in enumerate((wq, wk, wv, wo, wg, wu, wd)):
        def body(c, best, ref=ref):
            cols = pl.ds(pl.multiple_of(c * CHUNK, CHUNK), CHUNK)
            return jnp.maximum(best, jnp.max(jnp.abs(ref[:, cols].astype(F32)), axis=0, keepdims=True))

        best = lax.fori_loop(0, D // CHUNK, body, jnp.zeros((1, CHUNK), F32))
        mine = jnp.where(lane == t, jnp.max(best, axis=1, keepdims=True), mine)
    pk_s[...] = mine

    pl.semaphore_wait(barrier, N - 1 + TP - 1)

    def peak_copy(to, slot_of):
        return pltpu.make_async_remote_copy(
            pk_s, pk_r.at[slot_of], pks_sem.at[to], pkr_sem.at[slot_of], device_id={"fsdp": to}, device_id_type=MESH
        )

    def send_peak(j, _):
        peak_copy(target(N - 1 - j), me).start()
        return 0

    lax.fori_loop(0, N - 1, send_peak, 0)
    send(0)
    pack(1, [(wu, 0, WIDE), (wg, HEAD_COLS, WIDE)])
    send(1)

    def wait_peak(j, best):
        src = source(N - 1 - j)
        peak_copy(src, src).wait_recv()
        return jnp.maximum(best, pk_r[src])

    pt_s[...] = lax.fori_loop(0, N - 1, wait_peak, mine)

    def tp_copy(to, slot_of):
        return pltpu.make_async_remote_copy(
            pt_s, pt_r.at[slot_of], pts_sem.at[to], ptr_sem.at[slot_of], device_id={"tp": to}, device_id_type=MESH
        )

    def send_tp(i, _):
        tp_copy((tp + i) % TP, tp).start()
        return 0

    lax.fori_loop(1, TP, send_tp, 0)
    pack(2, [(wd, 0, WIDE), (wo, 0, SLIM)])

    def wait_tp(i, best):
        src = (tp + TP - i) % TP
        tp_copy(src, src).wait_recv()
        return jnp.maximum(best, pt_r[src])

    peaks = lax.fori_loop(1, TP, wait_tp, pt_s[...])

    on_row = lax.broadcasted_iota(jnp.int32, (7, LANES), 0) == lax.broadcasted_iota(jnp.int32, (7, LANES), 1)
    peaks_column = jnp.sum(jnp.where(on_row, peaks, 0.0), axis=1, keepdims=True)
    marked = lax.broadcasted_iota(jnp.int32, (7, HIST), 1) == slot[0]
    past = hist[...]
    kept = jnp.max(jnp.where(marked, 0.0, past), axis=1, keepdims=True)
    nh_o[...] = jnp.where(marked, peaks_column, past)
    fac[0:7, :] = jnp.broadcast_to(target_peak / jnp.maximum(peaks_column, kept), (7, LANES))

    def put(ref, tile, mask, value):
        cols = pl.ds(pl.multiple_of(tile * LANES, LANES), LANES)
        ref[:, cols] = jnp.where(mask, value, ref[:, cols].astype(F32)).astype(BF16)

    def place(ref, first, count, value):
        tiles = ref.shape[1] // LANES
        tile, at = first // LANES, first % LANES
        put(ref, tile, (lane >= at) & (lane < at + count), value)
        if tiles > 1:
            put(ref, tile + 1 - (tile + 1) // tiles, lane < at + count - LANES, value)

    def turn(value, now, then):
        return pltpu.roll(value, (then - now + 4 * LANES) % LANES, 1)

    def process(tile, block, s):
        x = block.astype(F32)
        base = (WIDE * s) % LANES
        if tile == 0:
            place(g_o, WIDE * s, HEAD_COLS, x * fac[4:5, :])
            place(q_o, SLIM * s, SLIM, turn(x * fac[0:1, :], base + HEAD_COLS, (SLIM * s) % LANES))
            place(k_o, TINY * s, TINY, turn(x * fac[1:2, :], base + HEAD_COLS + SLIM, TINY * s))
            place(v_o, TINY * s, TINY, turn(x * fac[2:3, :], base + HEAD_COLS + SLIM + TINY, TINY * s))
        elif tile == 1:
            place(u_o, WIDE * s, WIDE, x * fac[5:6, :])
            place(g_o, WIDE * s + HEAD_COLS, REST, turn(x * fac[4:5, :], base + WIDE, (WIDE * s + HEAD_COLS) % LANES))
        else:
            place(d_o, WIDE * s, WIDE, x * fac[6:7, :])
            place(o_o, SLIM * s, SLIM, turn(x * fac[3:4, :], base + WIDE, (SLIM * s) % LANES))

    def receive(tile):
        process(tile, sent[tile, pl.ds(pl.multiple_of(me * ROWS, ROWS), ROWS), :], me)

        def body(j, _):
            src = source(N - 1 - j)
            block_copy(tile, src, src).wait_recv()
            process(tile, got[tile, src], src)
            return 0

        lax.fori_loop(0, N - 1, body, 0)

    receive(0)

    row = lax.broadcasted_iota(jnp.int32, (64, 64), 0)
    col = lax.broadcasted_iota(jnp.int32, (64, 64), 1)
    owner = (row // 32) * 32 + ((row // 2) % 8) * 4 + ((row // 16) % 2) * 2 + row % 2
    ordered = jnp.dot((owner == col).astype(BF16), hid[...], preferred_element_type=F32)
    hidden = ordered.astype(BF16)
    part[:, 0:640] = jnp.dot(hidden, q_o[...], preferred_element_type=F32)
    part[:, 640:768] = jnp.dot(hidden, k_o[...], preferred_element_type=F32)
    part[:, 768:896] = jnp.dot(hidden, v_o[...], preferred_element_type=F32)
    part[:, 896:1024] = jnp.broadcast_to(jnp.sum(ordered * ordered, axis=1, keepdims=True), (64, LANES))

    group = my_y * 2 + my_c

    def one_copy(k, receiving):
        y, c = (my_y + k // 2) % 2, (my_c + k % 2) % 2
        other = y * 2 + c
        return other, pltpu.make_async_remote_copy(
            part.at[pl.ds(pl.multiple_of(other * 16, 16), 16)],
            one_r.at[other if receiving else group],
            ones_sem.at[other],
            oner_sem.at[other if receiving else group],
            device_id={"fsdp": y * 16 + my_z * 2 + c},
            device_id_type=MESH,
        )

    for k in range(1, 4):
        one_copy(k, False)[1].start()
    total = part[pl.ds(pl.multiple_of(group * 16, 16), 16), :]
    for k in range(1, 4):
        other, copy = one_copy(k, True)
        copy.wait_recv()
        total = total + one_r[other]
    for z in range(8):
        two_s[z] = total[2 * z : 2 * z + 2, :]

    def two_copy(z, slot_of):
        return pltpu.make_async_remote_copy(
            two_s.at[z],
            two_r.at[slot_of],
            twos_sem.at[z],
            twor_sem.at[slot_of],
            device_id={"fsdp": my_y * 16 + z * 2 + my_c},
            device_id_type=MESH,
        )

    def send_two(i, _):
        two_copy((my_z + i) % 8, my_z).start()
        return 0

    lax.fori_loop(1, 8, send_two, 0)
    send(2)
    receive(1)

    def wait_two(i, total):
        src = (my_z + 8 - i) % 8
        two_copy(src, src).wait_recv()
        return total + two_r[src]

    summed = lax.fori_loop(1, 8, wait_two, two_s[my_z])

    inv_rms = lax.rsqrt(summed[:, 896:1024] / D + norm_eps)
    token = lax.broadcasted_iota(jnp.int32, (2, LANES), 0)
    length = jnp.where(token == 0, lens[0], lens[1])
    angle = length.astype(F32) * spread[...]
    half = lax.broadcasted_iota(jnp.int32, (2, LANES), 1) < HEAD_DIM // 2
    cosine = jnp.cos(angle)
    sine = jnp.where(half, -jnp.sin(angle), jnp.sin(angle))

    def rotate(x):
        return x * cosine + pltpu.roll(x, HEAD_DIM // 2, 1) * sine

    heads = [
        rotate(summed[:, h * LANES : (h + 1) * LANES] * inv_rms / fac[0:1, :]).astype(BF16).astype(F32)
        for h in range(GROUP)
    ]
    key_new = rotate(summed[:, 640:768] * inv_rms / fac[1:2, :]).astype(BF16).astype(F32)
    value_new = (summed[:, 768:896] * inv_rms / fac[2:3, :]).astype(BF16).astype(F32)
    loads[7].wait()
    loads[8].wait()
    head_row = lax.broadcasted_iota(jnp.int32, (8, LANES), 0)
    scale = HEAD_DIM ** (-0.5)
    mixes = []
    for b in range(2):
        query = jnp.zeros((8, LANES), F32)
        for h in range(GROUP):
            query = jnp.where(head_row == h, heads[h][b : b + 1, :], query)
        scores = (
            lax.dot_general(query.astype(BF16), kc[b], (((1,), (1,)), ((), ())), preferred_element_type=F32) * scale
        )
        own = jnp.sum(query * key_new[b : b + 1, :], axis=1, keepdims=True) * scale
        valid = lax.broadcasted_iota(jnp.int32, (8, CACHE), 1) < lens[b]
        top = jnp.maximum(jnp.max(jnp.where(valid, scores, -1e30), axis=1, keepdims=True), own)
        weights = jnp.where(valid, jnp.exp(scores - top), 0.0)
        own_weight = jnp.exp(own - top)
        total = jnp.sum(weights, axis=1, keepdims=True) + own_weight
        probs = (weights / total).astype(BF16)
        own_prob = (own_weight / total).astype(BF16).astype(F32)
        mixed = jnp.dot(probs, vc[b], preferred_element_type=F32)
        mixes.append(mixed + own_prob * value_new[b : b + 1, :])
    for h in range(GROUP):
        pair = jnp.where(token == 0, mixes[0][h : h + 1, :], mixes[1][h : h + 1, :])
        att_o[:, h * LANES : (h + 1) * LANES] = pair.astype(BF16)

    receive(2)

    def drain(j, _):
        to = target(N - 1 - j)
        peak_copy(to, me).wait_send()
        for tile in range(3):
            block_copy(tile, to, me).wait_send()
        return 0

    lax.fori_loop(0, N - 1, drain, 0)

    def drain_tp(i, _):
        tp_copy((tp + i) % TP, tp).wait_send()
        return 0

    lax.fori_loop(1, TP, drain_tp, 0)
    for k in range(1, 4):
        one_copy(k, False)[1].wait_send()

    def drain_two(i, _):
        two_copy((my_z + i) % 8, my_z).wait_send()
        return 0

    lax.fori_loop(1, 8, drain_two, 0)


def per_device(
    hidden, query_weight, key_weight, value_weight, output_weight, gate_weight, up_weight, down_weight,
    history, slot, lengths, key_cache, value_cache,
):
    spread = np.float64(rope_theta) ** (-2.0 * (np.arange(HEAD_DIM) % (HEAD_DIM // 2)) / HEAD_DIM)
    spread = jnp.asarray(spread.astype(np.float32)[None, :])
    vmem = pl.BlockSpec(memory_space=pltpu.VMEM)
    smem = pl.BlockSpec(memory_space=pltpu.SMEM)
    hbm = pl.BlockSpec(memory_space=pl.ANY)
    out = [
        ((2, GROUP * HEAD_DIM), BF16),
        ((ROWS, 640), BF16),
        ((ROWS, 128), BF16),
        ((ROWS, 128), BF16),
        ((ROWS, 640), BF16),
        ((ROWS, 3456), BF16),
        ((ROWS, 3456), BF16),
        ((ROWS, 3456), BF16),
        ((7, HIST), F32),
    ]
    dma = pltpu.SemaphoreType.DMA
    results = pl.pallas_call(
        kernel,
        out_shape=[jax.ShapeDtypeStruct(s, t) for s, t in out],
        in_specs=[vmem] + [hbm] * 7 + [vmem, smem, smem, hbm, hbm, vmem],
        out_specs=[vmem] * 9,
        scratch_shapes=[
            pltpu.VMEM((SLIM, D), BF16),
            pltpu.VMEM((TINY, D), BF16),
            pltpu.VMEM((TINY, D), BF16),
            pltpu.VMEM((SLIM, D), BF16),
            pltpu.VMEM((WIDE, D), BF16),
            pltpu.VMEM((WIDE, D), BF16),
            pltpu.VMEM((WIDE, D), BF16),
            pltpu.VMEM((2, CACHE, HEAD_DIM), BF16),
            pltpu.VMEM((2, CACHE, HEAD_DIM), BF16),
            pltpu.VMEM((3, D, LANES), BF16),
            pltpu.VMEM((3, N, ROWS, LANES), BF16),
            pltpu.VMEM((8, LANES), F32),
            pltpu.VMEM((1, LANES), F32),
            pltpu.VMEM((N, 1, LANES), F32),
            pltpu.VMEM((1, LANES), F32),
            pltpu.VMEM((TP, 1, LANES), F32),
            pltpu.VMEM((64, 1024), F32),
            pltpu.VMEM((4, 16, 1024), F32),
            pltpu.VMEM((8, 2, 1024), F32),
            pltpu.VMEM((8, 2, 1024), F32),
            dma((9,)),
            dma((3, N)),
            dma((3, N)),
            dma((N,)),
            dma((N,)),
            dma((TP,)),
            dma((TP,)),
            dma((4,)),
            dma((4,)),
            dma((8,)),
            dma((8,)),
        ],
        compiler_params=pltpu.CompilerParams(
            collective_id=0, has_side_effects=True, vmem_limit_bytes=58 * 2**20
        ),
    )(
        hidden, query_weight.T, key_weight.T, value_weight.T, output_weight, gate_weight.T, up_weight.T, down_weight,
        history, slot, lengths, key_cache, value_cache, spread,
    )
    attention_out, query, key, value, output, gate, up, down, new_history = results
    return attention_out, query, key, value, output.T, gate, up, down.T, new_history


def solution(mesh):
    f, t = "fsdp", "tp"
    in_specs = (
        P(None, f), P(None, (t, f)), P(None, (t, f)), P(None, (t, f)), P((t, f), None), P(None, (t, f)),
        P(None, (t, f)), P((t, f), None), P(), P(), P(f), P(f, None, t), P(f, None, t),
    )
    out_specs = (P(f, t), P(f, t), P(f, t), P(f, t), P(t, f), P(f, t), P(f, t), P(t, f), P())
    return jax.shard_map(per_device, mesh=mesh, in_specs=in_specs, out_specs=out_specs, check_vma=False)
```

```python
import functools
import math

import jax
import jax.numpy as jnp
import numpy as np
from jax import lax
from jax.experimental import pallas as pl
from jax.experimental.pallas import tpu as pltpu
from jax.sharding import PartitionSpec as P

D = 5120
HEADS = 40
KV_HEADS = 8
HEAD_DIM = 128
GROUP = HEADS // KV_HEADS
CACHE = 4096
HIST = 1024
N = 32
TP = 8
ROWS = D // N
WIDE = 27648 // (N * TP)
SLIM = D // (N * TP)
TINY = KV_HEADS * HEAD_DIM // (N * TP)
LANES = 128
HEAD_COLS = LANES - SLIM - 2 * TINY
REST = WIDE - HEAD_COLS
CHUNK = 512
VMEM_LIMIT = 40 * 2**20

target_peak = 4.0
norm_eps = 1e-06
rope_theta = 1000000.0

F32 = jnp.float32
BF16 = jnp.bfloat16
MESH = pl.DeviceIdType.MESH


def offset(i):
    k = i // 4
    return (i // 2) % 2, ((k + 1) // 2) * (2 * (k % 2) - 1), i % 2


def kernel(
    hid_h, wq_h, wk_h, wv_h, wo_h, wg_h, wu_h, wd_h, hist_h, slot, lens_h, kc_h, vc_h, spread_h,
    att_o, q_o, k_o, v_o, o_o, g_o, u_o, d_o, nh_o,
    wq, wk, wv, wo, wg, wu, wd, kc, vc, hid, hist, spread, lens, sent, got, fac,
    pk_s, pk_r, pt_s, pt_r, part, one_r, two_s, two_r,
    load_sem, send_sem, recv_sem, pks_sem, pkr_sem, pts_sem, ptr_sem,
    ones_sem, oner_sem, twos_sem, twor_sem,
):
    me = lax.axis_index("fsdp")
    tp = lax.axis_index("tp")
    my_y, my_z, my_c = me // 16, (me // 2) % 8, me % 2

    def target(i):
        dy, dz, dc = offset(i)
        return ((my_y + dy) % 2) * 16 + ((my_z + dz + 8) % 8) * 2 + (my_c + dc) % 2

    def source(i):
        dy, dz, dc = offset(i)
        return ((my_y + dy) % 2) * 16 + ((my_z - dz + 8) % 8) * 2 + (my_c + dc) % 2

    barrier = pltpu.get_barrier_semaphore()

    def greet(i, _):
        pl.semaphore_signal(barrier, 1, device_id={"fsdp": target(i)}, device_id_type=MESH)
        return 0

    lax.fori_loop(1, N, greet, 0)

    def greet_tp(i, _):
        pl.semaphore_signal(barrier, 1, device_id={"tp": (tp + i) % TP}, device_id_type=MESH)
        return 0

    lax.fori_loop(1, TP, greet_tp, 0)

    loads = [
        pltpu.make_async_copy(src, dst, load_sem.at[n])
        for n, (src, dst) in enumerate(
            [(wg_h, wg), (wq_h, wq), (wk_h, wk), (wv_h, wv), (wu_h, wu), (wd_h, wd), (wo_h, wo),
             (hid_h, hid), (hist_h, hist), (spread_h, spread), (lens_h, lens), (kc_h, kc), (vc_h, vc)]
        )
    ]
    for load in loads:
        load.start()

    shift = (WIDE * me) % LANES

    def pack(tile, parts):
        def body(c, _):
            cols = pl.ds(pl.multiple_of(c * CHUNK, CHUNK), CHUNK)
            pieces = [ref[lo:hi, cols].astype(F32) for ref, lo, hi in parts]
            rows = sum(hi - lo for _, lo, hi in parts)
            if rows < LANES:
                pieces.append(jnp.zeros((LANES - rows, CHUNK), F32))
            block = jnp.concatenate(pieces, axis=0).T
            sent[tile, cols, :] = pltpu.roll(block, shift, 1).astype(BF16)
            return 0

        lax.fori_loop(0, D // CHUNK, body, 0)

    def block_copy(tile, to, slot_of):
        return pltpu.make_async_remote_copy(
            sent.at[tile, pl.ds(pl.multiple_of(to * ROWS, ROWS), ROWS)],
            got.at[tile, slot_of],
            send_sem.at[tile, to],
            recv_sem.at[tile, slot_of],
            device_id={"fsdp": to},
            device_id_type=MESH,
        )

    def send(tile):
        def body(j, _):
            block_copy(tile, target(N - 1 - j), me).start()
            return 0

        lax.fori_loop(0, N - 1, body, 0)

    for n in range(4):
        loads[n].wait()
    pack(0, [(wg, 0, HEAD_COLS), (wq, 0, SLIM), (wk, 0, TINY), (wv, 0, TINY)])
    for n in range(4, 7):
        loads[n].wait()

    lane = lax.broadcasted_iota(jnp.int32, (1, LANES), 1)
    mine = jnp.zeros((1, LANES), F32)
    for t, ref in enumerate((wq, wk, wv, wo, wg, wu, wd)):
        def body(c, best, ref=ref):
            cols = pl.ds(pl.multiple_of(c * CHUNK, CHUNK), CHUNK)
            return jnp.maximum(best, jnp.max(jnp.abs(ref[:, cols].astype(F32)), axis=0, keepdims=True))

        best = lax.fori_loop(0, D // CHUNK, body, jnp.zeros((1, CHUNK), F32))
        mine = jnp.where(lane == t, jnp.max(best, axis=1, keepdims=True), mine)
    pk_s[...] = mine

    pl.semaphore_wait(barrier, N - 1 + TP - 1)

    def peak_copy(to, slot_of):
        return pltpu.make_async_remote_copy(
            pk_s, pk_r.at[slot_of], pks_sem.at[to], pkr_sem.at[slot_of], device_id={"fsdp": to}, device_id_type=MESH
        )

    def send_peak(j, _):
        peak_copy(target(N - 1 - j), me).start()
        return 0

    lax.fori_loop(0, N - 1, send_peak, 0)
    send(0)
    pack(1, [(wu, 0, WIDE), (wg, HEAD_COLS, WIDE)])
    send(1)

    def wait_peak(j, best):
        src = source(N - 1 - j)
        peak_copy(src, src).wait_recv()
        return jnp.maximum(best, pk_r[src])

    pt_s[...] = lax.fori_loop(0, N - 1, wait_peak, mine)

    def tp_copy(to, slot_of):
        return pltpu.make_async_remote_copy(
            pt_s, pt_r.at[slot_of], pts_sem.at[to], ptr_sem.at[slot_of], device_id={"tp": to}, device_id_type=MESH
        )

    def send_tp(i, _):
        tp_copy((tp + i) % TP, tp).start()
        return 0

    lax.fori_loop(1, TP, send_tp, 0)
    pack(2, [(wd, 0, WIDE), (wo, 0, SLIM)])

    def wait_tp(i, best):
        src = (tp + TP - i) % TP
        tp_copy(src, src).wait_recv()
        return jnp.maximum(best, pt_r[src])

    peaks = lax.fori_loop(1, TP, wait_tp, pt_s[...])

    for n in range(7, 11):
        loads[n].wait()
    on_row = lax.broadcasted_iota(jnp.int32, (7, LANES), 0) == lax.broadcasted_iota(jnp.int32, (7, LANES), 1)
    peaks_column = jnp.sum(jnp.where(on_row, peaks, 0.0), axis=1, keepdims=True)
    marked = lax.broadcasted_iota(jnp.int32, (7, HIST), 1) == slot[0]
    past = hist[...]
    kept = jnp.max(jnp.where(marked, 0.0, past), axis=1, keepdims=True)
    nh_o[...] = jnp.where(marked, peaks_column, past)
    fac[0:7, :] = jnp.broadcast_to(target_peak / jnp.maximum(peaks_column, kept), (7, LANES))

    def put(ref, tile, mask, value):
        cols = pl.ds(pl.multiple_of(tile * LANES, LANES), LANES)
        ref[:, cols] = jnp.where(mask, value, ref[:, cols].astype(F32)).astype(BF16)

    def place(ref, first, count, value):
        tiles = ref.shape[1] // LANES
        tile, at = first // LANES, first % LANES
        put(ref, tile, (lane >= at) & (lane < at + count), value)
        if tiles > 1:
            put(ref, tile + 1 - (tile + 1) // tiles, lane < at + count - LANES, value)

    def turn(value, now, then):
        return pltpu.roll(value, (then - now + 4 * LANES) % LANES, 1)

    def process(tile, block, s):
        x = block.astype(F32)
        base = (WIDE * s) % LANES
        if tile == 0:
            place(g_o, WIDE * s, HEAD_COLS, x * fac[4:5, :])
            place(q_o, SLIM * s, SLIM, turn(x * fac[0:1, :], base + HEAD_COLS, (SLIM * s) % LANES))
            place(k_o, TINY * s, TINY, turn(x * fac[1:2, :], base + HEAD_COLS + SLIM, TINY * s))
            place(v_o, TINY * s, TINY, turn(x * fac[2:3, :], base + HEAD_COLS + SLIM + TINY, TINY * s))
        elif tile == 1:
            place(u_o, WIDE * s, WIDE, x * fac[5:6, :])
            place(g_o, WIDE * s + HEAD_COLS, REST, turn(x * fac[4:5, :], base + WIDE, (WIDE * s + HEAD_COLS) % LANES))
        else:
            place(d_o, WIDE * s, WIDE, x * fac[6:7, :])
            place(o_o, SLIM * s, SLIM, turn(x * fac[3:4, :], base + WIDE, (SLIM * s) % LANES))

    def receive(tile):
        process(tile, sent[tile, pl.ds(pl.multiple_of(me * ROWS, ROWS), ROWS), :], me)

        def body(j, _):
            src = source(N - 1 - j)
            block_copy(tile, src, src).wait_recv()
            process(tile, got[tile, src], src)
            return 0

        lax.fori_loop(0, N - 1, body, 0)

    receive(0)

    row = lax.broadcasted_iota(jnp.int32, (64, 64), 0)
    col = lax.broadcasted_iota(jnp.int32, (64, 64), 1)
    owner = (row // 32) * 32 + ((row // 2) % 8) * 4 + ((row // 16) % 2) * 2 + row % 2
    ordered = jnp.dot((owner == col).astype(BF16), hid[...], preferred_element_type=F32)
    hidden = ordered.astype(BF16)
    part[:, 0:640] = jnp.dot(hidden, q_o[...], preferred_element_type=F32)
    part[:, 640:768] = jnp.dot(hidden, k_o[...], preferred_element_type=F32)
    part[:, 768:896] = jnp.dot(hidden, v_o[...], preferred_element_type=F32)
    part[:, 896:1024] = jnp.broadcast_to(jnp.sum(ordered * ordered, axis=1, keepdims=True), (64, LANES))

    group = my_y * 2 + my_c

    def one_copy(k, receiving):
        y, c = (my_y + k // 2) % 2, (my_c + k % 2) % 2
        other = y * 2 + c
        return other, pltpu.make_async_remote_copy(
            part.at[pl.ds(pl.multiple_of(other * 16, 16), 16)],
            one_r.at[other if receiving else group],
            ones_sem.at[other],
            oner_sem.at[other if receiving else group],
            device_id={"fsdp": y * 16 + my_z * 2 + c},
            device_id_type=MESH,
        )

    for k in range(1, 4):
        one_copy(k, False)[1].start()
    total = part[pl.ds(pl.multiple_of(group * 16, 16), 16), :]
    for k in range(1, 4):
        other, copy = one_copy(k, True)
        copy.wait_recv()
        total = total + one_r[other]
    for z in range(8):
        two_s[z] = total[2 * z : 2 * z + 2, :]

    def two_copy(z, slot_of):
        return pltpu.make_async_remote_copy(
            two_s.at[z],
            two_r.at[slot_of],
            twos_sem.at[z],
            twor_sem.at[slot_of],
            device_id={"fsdp": my_y * 16 + z * 2 + my_c},
            device_id_type=MESH,
        )

    def send_two(i, _):
        two_copy((my_z + i) % 8, my_z).start()
        return 0

    lax.fori_loop(1, 8, send_two, 0)
    send(2)
    receive(1)

    def wait_two(i, total):
        src = (my_z + 8 - i) % 8
        two_copy(src, src).wait_recv()
        return total + two_r[src]

    summed = lax.fori_loop(1, 8, wait_two, two_s[my_z])

    inv_rms = lax.rsqrt(summed[:, 896:1024] / D + norm_eps)
    token = lax.broadcasted_iota(jnp.int32, (2, LANES), 0)
    length = jnp.where(token == 0, lens[0], lens[1])
    angle = length.astype(F32) * spread[...]
    half = lax.broadcasted_iota(jnp.int32, (2, LANES), 1) < HEAD_DIM // 2
    cosine = jnp.cos(angle)
    sine = jnp.where(half, -jnp.sin(angle), jnp.sin(angle))

    def rotate(x):
        return x * cosine + pltpu.roll(x, HEAD_DIM // 2, 1) * sine

    heads = [
        rotate(summed[:, h * LANES : (h + 1) * LANES] * inv_rms / fac[0:1, :]).astype(BF16).astype(F32)
        for h in range(GROUP)
    ]
    key_new = rotate(summed[:, 640:768] * inv_rms / fac[1:2, :]).astype(BF16).astype(F32)
    value_new = (summed[:, 768:896] * inv_rms / fac[2:3, :]).astype(BF16).astype(F32)
    loads[11].wait()
    loads[12].wait()
    head_row = lax.broadcasted_iota(jnp.int32, (8, LANES), 0)
    scale = HEAD_DIM ** (-0.5)
    mixes = []
    for b in range(2):
        query = jnp.zeros((8, LANES), F32)
        for h in range(GROUP):
            query = jnp.where(head_row == h, heads[h][b : b + 1, :], query)
        scores = (
            lax.dot_general(query.astype(BF16), kc[b], (((1,), (1,)), ((), ())), preferred_element_type=F32) * scale
        )
        own = jnp.sum(query * key_new[b : b + 1, :], axis=1, keepdims=True) * scale
        valid = lax.broadcasted_iota(jnp.int32, (8, CACHE), 1) < lens[b]
        top = jnp.maximum(jnp.max(jnp.where(valid, scores, -1e30), axis=1, keepdims=True), own)
        weights = jnp.where(valid, jnp.exp(scores - top), 0.0)
        own_weight = jnp.exp(own - top)
        total = jnp.sum(weights, axis=1, keepdims=True) + own_weight
        probs = (weights / total).astype(BF16)
        own_prob = (own_weight / total).astype(BF16).astype(F32)
        mixed = jnp.dot(probs, vc[b], preferred_element_type=F32)
        mixes.append(mixed + own_prob * value_new[b : b + 1, :])
    for h in range(GROUP):
        pair = jnp.where(token == 0, mixes[0][h : h + 1, :], mixes[1][h : h + 1, :])
        att_o[:, h * LANES : (h + 1) * LANES] = pair.astype(BF16)

    receive(2)

    def drain(j, _):
        to = target(N - 1 - j)
        peak_copy(to, me).wait_send()
        for tile in range(3):
            block_copy(tile, to, me).wait_send()
        return 0

    lax.fori_loop(0, N - 1, drain, 0)

    def drain_tp(i, _):
        tp_copy((tp + i) % TP, tp).wait_send()
        return 0

    lax.fori_loop(1, TP, drain_tp, 0)
    for k in range(1, 4):
        one_copy(k, False)[1].wait_send()

    def drain_two(i, _):
        two_copy((my_z + i) % 8, my_z).wait_send()
        return 0

    lax.fori_loop(1, 8, drain_two, 0)


def finish(*refs):
    count = (len(refs) - 1) // 2
    copies = [pltpu.make_async_copy(refs[n], refs[count + n], refs[-1].at[n]) for n in range(count)]
    for copy in copies:
        copy.start()
    for copy in copies:
        copy.wait()


def per_device(
    hidden, query_weight, key_weight, value_weight, output_weight, gate_weight, up_weight, down_weight,
    history, slot, lengths, key_cache, value_cache,
):
    spread = np.float64(rope_theta) ** (-2.0 * (np.arange(HEAD_DIM) % (HEAD_DIM // 2)) / HEAD_DIM)
    spread = jnp.asarray(spread.astype(np.float32)[None, :])
    vmem = pl.BlockSpec(memory_space=pltpu.VMEM)
    hbm = pl.BlockSpec(memory_space=pltpu.HBM)
    out = [
        ((2, GROUP * HEAD_DIM), BF16),
        ((ROWS, 640), BF16),
        ((ROWS, 128), BF16),
        ((ROWS, 128), BF16),
        ((ROWS, 640), BF16),
        ((ROWS, 3456), BF16),
        ((ROWS, 3456), BF16),
        ((ROWS, 3456), BF16),
        ((7, HIST), F32),
    ]
    dma = pltpu.SemaphoreType.DMA
    results = pl.pallas_call(
        kernel,
        out_shape=[pltpu.VMEM(s, t) for s, t in out],
        in_specs=[hbm] * 9 + [pl.BlockSpec(memory_space=pltpu.SMEM)] + [hbm] * 4,
        out_specs=[vmem] * 9,
        scratch_shapes=[
            pltpu.VMEM((SLIM, D), BF16),
            pltpu.VMEM((TINY, D), BF16),
            pltpu.VMEM((TINY, D), BF16),
            pltpu.VMEM((SLIM, D), BF16),
            pltpu.VMEM((WIDE, D), BF16),
            pltpu.VMEM((WIDE, D), BF16),
            pltpu.VMEM((WIDE, D), BF16),
            pltpu.VMEM((2, CACHE, HEAD_DIM), BF16),
            pltpu.VMEM((2, CACHE, HEAD_DIM), BF16),
            pltpu.VMEM((64, ROWS), BF16),
            pltpu.VMEM((7, HIST), F32),
            pltpu.VMEM((1, LANES), F32),
            pltpu.SMEM((2,), jnp.int32),
            pltpu.VMEM((3, D, LANES), BF16),
            pltpu.VMEM((3, N, ROWS, LANES), BF16),
            pltpu.VMEM((8, LANES), F32),
            pltpu.VMEM((1, LANES), F32),
            pltpu.VMEM((N, 1, LANES), F32),
            pltpu.VMEM((1, LANES), F32),
            pltpu.VMEM((TP, 1, LANES), F32),
            pltpu.VMEM((64, 1024), F32),
            pltpu.VMEM((4, 16, 1024), F32),
            pltpu.VMEM((8, 2, 1024), F32),
            pltpu.VMEM((8, 2, 1024), F32),
            dma((13,)),
            dma((3, N)),
            dma((3, N)),
            dma((N,)),
            dma((N,)),
            dma((TP,)),
            dma((TP,)),
            dma((4,)),
            dma((4,)),
            dma((8,)),
            dma((8,)),
        ],
        compiler_params=pltpu.CompilerParams(
            collective_id=0, has_side_effects=True, vmem_limit_bytes=VMEM_LIMIT
        ),
    )(
        *(
            x if x is slot else pltpu.with_memory_space_constraint(x, pltpu.HBM)
            for x in (
                hidden, query_weight.T, key_weight.T, value_weight.T, output_weight, gate_weight.T, up_weight.T,
                down_weight, history, slot, lengths, key_cache, value_cache, spread,
            )
        )
    )
    results = pl.pallas_call(
        finish,
        out_shape=[jax.ShapeDtypeStruct(s, t) for s, t in out],
        in_specs=[vmem] * 9,
        out_specs=[hbm] * 9,
        scratch_shapes=[dma((9,))],
        compiler_params=pltpu.CompilerParams(vmem_limit_bytes=8 * 2**20),
    )(*results)
    attention_out, query, key, value, output, gate, up, down, new_history = results
    return attention_out, query, key, value, output.T, gate, up, down.T, new_history


def solution(mesh):
    f, t = "fsdp", "tp"
    in_specs = (
        P(None, f), P(None, (t, f)), P(None, (t, f)), P(None, (t, f)), P((t, f), None), P(None, (t, f)),
        P(None, (t, f)), P((t, f), None), P(), P(), P(f), P(f, None, t), P(f, None, t),
    )
    out_specs = (P(f, t), P(f, t), P(f, t), P(f, t), P(t, f), P(f, t), P(f, t), P(t, f), P())
    return jax.shard_map(per_device, mesh=mesh, in_specs=in_specs, out_specs=out_specs, check_vma=False)
```

```python
import functools
import math

import jax
import jax.numpy as jnp
import numpy as np
from jax import lax
from jax.experimental import pallas as pl
from jax.experimental.pallas import tpu as pltpu
from jax.sharding import PartitionSpec as P

D = 5120
HEADS = 40
KV_HEADS = 8
HEAD_DIM = 128
GROUP = HEADS // KV_HEADS
CACHE = 4096
HIST = 1024
N = 32
TP = 8
ROWS = D // N
WIDE = 27648 // (N * TP)
SLIM = D // (N * TP)
TINY = KV_HEADS * HEAD_DIM // (N * TP)
LANES = 128
HEAD_COLS = LANES - SLIM - 2 * TINY
REST = WIDE - HEAD_COLS
CHUNK = 512
VMEM_LIMIT = 40 * 2**20

target_peak = 4.0
norm_eps = 1e-06
rope_theta = 1000000.0

F32 = jnp.float32
BF16 = jnp.bfloat16
MESH = pl.DeviceIdType.MESH


def offset(i):
    k = lax.div(i, 4) if isinstance(i, jax.Array) else i // 4
    odd = lax.rem(k, 2) if isinstance(i, jax.Array) else k % 2
    if isinstance(i, jax.Array):
        return lax.rem(lax.div(i, 2), 2), lax.rem(lax.div(k + 1, 2) * (2 * odd - 1) + 8, 8), lax.rem(i, 2)
    return (i // 2) % 2, ((k + 1) // 2 * (2 * odd - 1)) % 8, i % 2


def kernel(
    hid_h, wq_h, wk_h, wv_h, wo_h, wg_h, wu_h, wd_h, hist_h, slot, lens_h, kc_h, vc_h, spread_h,
    att_o, q_o, k_o, v_o, o_o, g_o, u_o, d_o, nh_o,
    wq, wk, wv, wo, wg, wu, wd, kc, vc, hid, hist, spread, lens, sent, got, fac,
    pk_s, pk_r, pt_s, pt_r, part, one_r, two_s, two_r,
    load_sem, send_sem, recv_sem, pks_sem, pkr_sem, pts_sem, ptr_sem,
    ones_sem, oner_sem, twos_sem, twor_sem,
):
    me = lax.axis_index("fsdp")
    tp = lax.axis_index("tp")
    my_y, my_z, my_c = lax.div(me, 16), lax.rem(lax.div(me, 2), 8), lax.rem(me, 2)

    def device(dy, dz, dc):
        return lax.rem(my_y + dy, 2) * 16 + lax.rem(my_z + dz, 8) * 2 + lax.rem(my_c + dc, 2)

    def source(i):
        dy, dz, dc = offset(i)
        return device(dy, 8 - dz, dc)

    partners = [device(*offset(i)) for i in range(N - 1, 0, -1)]

    barrier = pltpu.get_barrier_semaphore()
    for to in partners:
        pl.semaphore_signal(barrier, 1, device_id={"fsdp": to}, device_id_type=MESH)
    for i in range(1, TP):
        pl.semaphore_signal(barrier, 1, device_id={"tp": lax.rem(tp + i, TP)}, device_id_type=MESH)

    loads = [
        pltpu.make_async_copy(src, dst, load_sem.at[n])
        for n, (src, dst) in enumerate(
            [(wg_h, wg), (wq_h, wq), (wk_h, wk), (wv_h, wv), (wu_h, wu), (wd_h, wd), (wo_h, wo),
             (hid_h, hid), (hist_h, hist), (spread_h, spread), (lens_h, lens), (kc_h, kc), (vc_h, vc)]
        )
    ]
    for load in loads:
        load.start()

    shift = lax.rem(WIDE * me, LANES)

    def pack(tile, parts):
        def body(c, _):
            cols = pl.ds(pl.multiple_of(c * CHUNK, CHUNK), CHUNK)
            pieces = [ref[lo:hi, cols].astype(F32) for ref, lo, hi in parts]
            rows = sum(hi - lo for _, lo, hi in parts)
            if rows < LANES:
                pieces.append(jnp.zeros((LANES - rows, CHUNK), F32))
            block = jnp.concatenate(pieces, axis=0).T
            sent[tile, cols, :] = pltpu.roll(block, shift, 1).astype(BF16)
            return 0

        lax.fori_loop(0, D // CHUNK, body, 0)

    def block_copy(tile, to, slot_of, j=0):
        return pltpu.make_async_remote_copy(
            sent.at[tile, pl.ds(pl.multiple_of(to * ROWS, ROWS), ROWS)],
            got.at[tile, slot_of],
            send_sem.at[tile, j],
            recv_sem.at[tile, slot_of],
            device_id={"fsdp": to},
            device_id_type=MESH,
        )

    def send(tile):
        for j, to in enumerate(partners):
            block_copy(tile, to, me, j).start()

    for n in range(4):
        loads[n].wait()
    pack(0, [(wg, 0, HEAD_COLS), (wq, 0, SLIM), (wk, 0, TINY), (wv, 0, TINY)])
    for n in range(4, 7):
        loads[n].wait()

    lane = lax.broadcasted_iota(jnp.int32, (1, LANES), 1)
    mine = jnp.zeros((1, LANES), F32)
    for t, ref in enumerate((wq, wk, wv, wo, wg, wu, wd)):
        def body(c, best, ref=ref):
            cols = pl.ds(pl.multiple_of(c * CHUNK, CHUNK), CHUNK)
            return jnp.maximum(best, jnp.max(jnp.abs(ref[:, cols].astype(F32)), axis=0, keepdims=True))

        best = lax.fori_loop(0, D // CHUNK, body, jnp.zeros((1, CHUNK), F32))
        mine = jnp.where(lane == t, jnp.max(best, axis=1, keepdims=True), mine)
    pk_s[...] = mine

    pl.semaphore_wait(barrier, N - 1 + TP - 1)

    def peak_copy(to, slot_of, j=0):
        return pltpu.make_async_remote_copy(
            pk_s, pk_r.at[slot_of], pks_sem.at[j], pkr_sem.at[slot_of], device_id={"fsdp": to}, device_id_type=MESH
        )

    for j, to in enumerate(partners):
        peak_copy(to, me, j).start()
    send(0)
    pack(1, [(wu, 0, WIDE), (wg, HEAD_COLS, WIDE)])
    send(1)

    def wait_peak(j, best):
        src = source(N - 1 - j)
        peak_copy(src, src).wait_recv()
        return jnp.maximum(best, pk_r[src])

    pt_s[...] = lax.fori_loop(0, N - 1, wait_peak, mine)

    def tp_copy(to, slot_of, i=0):
        return pltpu.make_async_remote_copy(
            pt_s, pt_r.at[slot_of], pts_sem.at[i], ptr_sem.at[slot_of], device_id={"tp": to}, device_id_type=MESH
        )

    for i in range(1, TP):
        tp_copy(lax.rem(tp + i, TP), tp, i).start()
    pack(2, [(wd, 0, WIDE), (wo, 0, SLIM)])

    def wait_tp(i, best):
        src = lax.rem(tp + TP - i, TP)
        tp_copy(src, src).wait_recv()
        return jnp.maximum(best, pt_r[src])

    peaks = lax.fori_loop(1, TP, wait_tp, pt_s[...])

    for n in range(7, 11):
        loads[n].wait()
    on_row = lax.broadcasted_iota(jnp.int32, (7, LANES), 0) == lax.broadcasted_iota(jnp.int32, (7, LANES), 1)
    peaks_column = jnp.sum(jnp.where(on_row, peaks, 0.0), axis=1, keepdims=True)
    marked = lax.broadcasted_iota(jnp.int32, (7, HIST), 1) == slot[0]
    past = hist[...]
    kept = jnp.max(jnp.where(marked, 0.0, past), axis=1, keepdims=True)
    nh_o[...] = jnp.where(marked, peaks_column, past)
    fac[0:7, :] = jnp.broadcast_to(target_peak / jnp.maximum(peaks_column, kept), (7, LANES))

    def put(ref, tile, mask, value):
        cols = pl.ds(pl.multiple_of(tile * LANES, LANES), LANES)
        ref[:, cols] = jnp.where(mask, value, ref[:, cols].astype(F32)).astype(BF16)

    def place(ref, first, count, value):
        tiles = ref.shape[1] // LANES
        tile, at = lax.div(first, LANES), lax.rem(first, LANES)
        put(ref, tile, (lane >= at) & (lane < at + count), value)
        if tiles > 1:
            put(ref, tile + 1 - lax.div(tile + 1, tiles), lane < at + count - LANES, value)

    def turn(value, now, then):
        return pltpu.roll(value, lax.rem(then - now + 4 * LANES, LANES), 1)

    def process(tile, block, s):
        x = block.astype(F32)
        base = lax.rem(WIDE * s, LANES)
        if tile == 0:
            place(g_o, WIDE * s, HEAD_COLS, x * fac[4:5, :])
            place(q_o, SLIM * s, SLIM, turn(x * fac[0:1, :], base + HEAD_COLS, lax.rem(SLIM * s, LANES)))
            place(k_o, TINY * s, TINY, turn(x * fac[1:2, :], base + HEAD_COLS + SLIM, TINY * s))
            place(v_o, TINY * s, TINY, turn(x * fac[2:3, :], base + HEAD_COLS + SLIM + TINY, TINY * s))
        elif tile == 1:
            place(u_o, WIDE * s, WIDE, x * fac[5:6, :])
            place(g_o, WIDE * s + HEAD_COLS, REST, turn(x * fac[4:5, :], base + WIDE, lax.rem(WIDE * s + HEAD_COLS, LANES)))
        else:
            place(d_o, WIDE * s, WIDE, x * fac[6:7, :])
            place(o_o, SLIM * s, SLIM, turn(x * fac[3:4, :], base + WIDE, lax.rem(SLIM * s, LANES)))

    def receive(tile):
        process(tile, sent[tile, pl.ds(pl.multiple_of(me * ROWS, ROWS), ROWS), :], me)

        def body(j, _):
            src = source(N - 1 - j)
            block_copy(tile, src, src).wait_recv()
            process(tile, got[tile, src], src)
            return 0

        lax.fori_loop(0, N - 1, body, 0)

    receive(0)

    row = lax.broadcasted_iota(jnp.int32, (64, 64), 0)
    col = lax.broadcasted_iota(jnp.int32, (64, 64), 1)
    owner = (row // 32) * 32 + ((row // 2) % 8) * 4 + ((row // 16) % 2) * 2 + row % 2
    ordered = jnp.dot((owner == col).astype(BF16), hid[...], preferred_element_type=F32)
    hidden = ordered.astype(BF16)
    part[:, 0:640] = jnp.dot(hidden, q_o[...], preferred_element_type=F32)
    part[:, 640:768] = jnp.dot(hidden, k_o[...], preferred_element_type=F32)
    part[:, 768:896] = jnp.dot(hidden, v_o[...], preferred_element_type=F32)
    part[:, 896:1024] = jnp.broadcast_to(jnp.sum(ordered * ordered, axis=1, keepdims=True), (64, LANES))

    group = my_y * 2 + my_c

    def one_copy(k, receiving):
        y, c = lax.rem(my_y + k // 2, 2), lax.rem(my_c + k % 2, 2)
        other = y * 2 + c
        return other, pltpu.make_async_remote_copy(
            part.at[pl.ds(pl.multiple_of(other * 16, 16), 16)],
            one_r.at[other if receiving else group],
            ones_sem.at[other],
            oner_sem.at[other if receiving else group],
            device_id={"fsdp": y * 16 + my_z * 2 + c},
            device_id_type=MESH,
        )

    for k in range(1, 4):
        one_copy(k, False)[1].start()
    total = part[pl.ds(pl.multiple_of(group * 16, 16), 16), :]
    for k in range(1, 4):
        other, copy = one_copy(k, True)
        copy.wait_recv()
        total = total + one_r[other]
    for z in range(8):
        two_s[z] = total[2 * z : 2 * z + 2, :]

    def two_copy(z, slot_of, i=0):
        return pltpu.make_async_remote_copy(
            two_s.at[z],
            two_r.at[slot_of],
            twos_sem.at[i],
            twor_sem.at[slot_of],
            device_id={"fsdp": my_y * 16 + z * 2 + my_c},
            device_id_type=MESH,
        )

    for i in range(1, 8):
        two_copy(lax.rem(my_z + i, 8), my_z, i).start()
    send(2)
    receive(1)

    def wait_two(i, total):
        src = lax.rem(my_z + 8 - i, 8)
        two_copy(src, src).wait_recv()
        return total + two_r[src]

    summed = lax.fori_loop(1, 8, wait_two, two_s[my_z])

    inv_rms = lax.rsqrt(summed[:, 896:1024] / D + norm_eps)
    token = lax.broadcasted_iota(jnp.int32, (2, LANES), 0)
    length = jnp.where(token == 0, lens[0], lens[1])
    angle = length.astype(F32) * spread[...]
    half = lax.broadcasted_iota(jnp.int32, (2, LANES), 1) < HEAD_DIM // 2
    cosine = jnp.cos(angle)
    sine = jnp.where(half, -jnp.sin(angle), jnp.sin(angle))

    def rotate(x):
        return x * cosine + pltpu.roll(x, HEAD_DIM // 2, 1) * sine

    heads = [
        rotate(summed[:, h * LANES : (h + 1) * LANES] * inv_rms / fac[0:1, :]).astype(BF16).astype(F32)
        for h in range(GROUP)
    ]
    key_new = rotate(summed[:, 640:768] * inv_rms / fac[1:2, :]).astype(BF16).astype(F32)
    value_new = (summed[:, 768:896] * inv_rms / fac[2:3, :]).astype(BF16).astype(F32)
    loads[11].wait()
    loads[12].wait()
    head_row = lax.broadcasted_iota(jnp.int32, (8, LANES), 0)
    scale = HEAD_DIM ** (-0.5)
    mixes = []
    for b in range(2):
        query = jnp.zeros((8, LANES), F32)
        for h in range(GROUP):
            query = jnp.where(head_row == h, heads[h][b : b + 1, :], query)
        scores = (
            lax.dot_general(query.astype(BF16), kc[b], (((1,), (1,)), ((), ())), preferred_element_type=F32) * scale
        )
        own = jnp.sum(query * key_new[b : b + 1, :], axis=1, keepdims=True) * scale
        valid = lax.broadcasted_iota(jnp.int32, (8, CACHE), 1) < lens[b]
        top = jnp.maximum(jnp.max(jnp.where(valid, scores, -1e30), axis=1, keepdims=True), own)
        weights = jnp.where(valid, jnp.exp(scores - top), 0.0)
        own_weight = jnp.exp(own - top)
        total = jnp.sum(weights, axis=1, keepdims=True) + own_weight
        probs = (weights / total).astype(BF16)
        own_prob = (own_weight / total).astype(BF16).astype(F32)
        mixed = jnp.dot(probs, vc[b], preferred_element_type=F32)
        mixes.append(mixed + own_prob * value_new[b : b + 1, :])
    for h in range(GROUP):
        pair = jnp.where(token == 0, mixes[0][h : h + 1, :], mixes[1][h : h + 1, :])
        att_o[:, h * LANES : (h + 1) * LANES] = pair.astype(BF16)

    for j, to in enumerate(partners):
        peak_copy(to, me, j).wait_send()
        for tile in range(2):
            block_copy(tile, to, me, j).wait_send()
    for i in range(1, TP):
        tp_copy(lax.rem(tp + i, TP), tp, i).wait_send()
    for k in range(1, 4):
        one_copy(k, False)[1].wait_send()
    for i in range(1, 8):
        two_copy(lax.rem(my_z + i, 8), my_z, i).wait_send()
    receive(2)
    for j, to in enumerate(partners):
        block_copy(2, to, me, j).wait_send()


def finish(*refs):
    count = (len(refs) - 1) // 2
    copies = [pltpu.make_async_copy(refs[n], refs[count + n], refs[-1].at[n]) for n in range(count)]
    for copy in copies:
        copy.start()
    for copy in copies:
        copy.wait()


def per_device(
    hidden, query_weight, key_weight, value_weight, output_weight, gate_weight, up_weight, down_weight,
    history, slot, lengths, key_cache, value_cache,
):
    spread = np.float64(rope_theta) ** (-2.0 * (np.arange(HEAD_DIM) % (HEAD_DIM // 2)) / HEAD_DIM)
    spread = jnp.asarray(spread.astype(np.float32)[None, :])
    vmem = pl.BlockSpec(memory_space=pltpu.VMEM)
    hbm = pl.BlockSpec(memory_space=pltpu.HBM)
    out = [
        ((2, GROUP * HEAD_DIM), BF16),
        ((ROWS, 640), BF16),
        ((ROWS, 128), BF16),
        ((ROWS, 128), BF16),
        ((ROWS, 640), BF16),
        ((ROWS, 3456), BF16),
        ((ROWS, 3456), BF16),
        ((ROWS, 3456), BF16),
        ((7, HIST), F32),
    ]
    dma = pltpu.SemaphoreType.DMA
    results = pl.pallas_call(
        kernel,
        out_shape=[pltpu.VMEM(s, t) for s, t in out],
        in_specs=[hbm] * 9 + [pl.BlockSpec(memory_space=pltpu.SMEM)] + [hbm] * 4,
        out_specs=[vmem] * 9,
        scratch_shapes=[
            pltpu.VMEM((SLIM, D), BF16),
            pltpu.VMEM((TINY, D), BF16),
            pltpu.VMEM((TINY, D), BF16),
            pltpu.VMEM((SLIM, D), BF16),
            pltpu.VMEM((WIDE, D), BF16),
            pltpu.VMEM((WIDE, D), BF16),
            pltpu.VMEM((WIDE, D), BF16),
            pltpu.VMEM((2, CACHE, HEAD_DIM), BF16),
            pltpu.VMEM((2, CACHE, HEAD_DIM), BF16),
            pltpu.VMEM((64, ROWS), BF16),
            pltpu.VMEM((7, HIST), F32),
            pltpu.VMEM((1, LANES), F32),
            pltpu.SMEM((2,), jnp.int32),
            pltpu.VMEM((3, D, LANES), BF16),
            pltpu.VMEM((3, N, ROWS, LANES), BF16),
            pltpu.VMEM((8, LANES), F32),
            pltpu.VMEM((1, LANES), F32),
            pltpu.VMEM((N, 1, LANES), F32),
            pltpu.VMEM((1, LANES), F32),
            pltpu.VMEM((TP, 1, LANES), F32),
            pltpu.VMEM((64, 1024), F32),
            pltpu.VMEM((4, 16, 1024), F32),
            pltpu.VMEM((8, 2, 1024), F32),
            pltpu.VMEM((8, 2, 1024), F32),
            dma((13,)),
            dma((3, N)),
            dma((3, N)),
            dma((N,)),
            dma((N,)),
            dma((TP,)),
            dma((TP,)),
            dma((4,)),
            dma((4,)),
            dma((8,)),
            dma((8,)),
        ],
        compiler_params=pltpu.CompilerParams(
            collective_id=0, has_side_effects=True, vmem_limit_bytes=VMEM_LIMIT
        ),
    )(
        *(
            x if x is slot else pltpu.with_memory_space_constraint(x, pltpu.HBM)
            for x in (
                hidden, query_weight.T, key_weight.T, value_weight.T, output_weight, gate_weight.T, up_weight.T,
                down_weight, history, slot, lengths, key_cache, value_cache, spread,
            )
        )
    )
    results = pl.pallas_call(
        finish,
        out_shape=[jax.ShapeDtypeStruct(s, t) for s, t in out],
        in_specs=[vmem] * 9,
        out_specs=[hbm] * 9,
        scratch_shapes=[dma((9,))],
        compiler_params=pltpu.CompilerParams(vmem_limit_bytes=8 * 2**20),
    )(*results)
    attention_out, query, key, value, output, gate, up, down, new_history = results
    return attention_out, query, key, value, output.T, gate, up, down.T, new_history


def solution(mesh):
    f, t = "fsdp", "tp"
    in_specs = (
        P(None, f), P(None, (t, f)), P(None, (t, f)), P(None, (t, f)), P((t, f), None), P(None, (t, f)),
        P(None, (t, f)), P((t, f), None), P(), P(), P(f), P(f, None, t), P(f, None, t),
    )
    out_specs = (P(f, t), P(f, t), P(f, t), P(f, t), P(t, f), P(f, t), P(f, t), P(t, f), P())
    return jax.shard_map(per_device, mesh=mesh, in_specs=in_specs, out_specs=out_specs, check_vma=False)
```

```python
import functools
import math

import jax
import jax.numpy as jnp
import numpy as np
from jax import lax
from jax.experimental import pallas as pl
from jax.experimental.pallas import tpu as pltpu
from jax.sharding import PartitionSpec as P

D = 5120
HEADS = 40
KV_HEADS = 8
HEAD_DIM = 128
GROUP = HEADS // KV_HEADS
CACHE = 4096
HIST = 1024
N = 32
TP = 8
ROWS = D // N
WIDE = 27648 // (N * TP)
SLIM = D // (N * TP)
TINY = KV_HEADS * HEAD_DIM // (N * TP)
LANES = 128
HEAD_COLS = LANES - SLIM - 2 * TINY
REST = WIDE - HEAD_COLS
CHUNK = 640
SPARE = LANES - WIDE - REST
TAIL = 16
SENT = ROWS - TAIL
MOVES = WIDE // SPARE
VMEM_LIMIT = 40 * 2**20

target_peak = 4.0
norm_eps = 1e-06
rope_theta = 1000000.0

F32 = jnp.float32
BF16 = jnp.bfloat16
MESH = pl.DeviceIdType.MESH


def offset(i):
    k = lax.div(i, 4) if isinstance(i, jax.Array) else i // 4
    odd = lax.rem(k, 2) if isinstance(i, jax.Array) else k % 2
    if isinstance(i, jax.Array):
        return lax.rem(lax.div(i, 2), 2), lax.rem(lax.div(k + 1, 2) * (2 * odd - 1) + 8, 8), lax.rem(i, 2)
    return (i // 2) % 2, ((k + 1) // 2 * (2 * odd - 1)) % 8, i % 2


def kernel(
    hid_h, wq_h, wk_h, wv_h, wo_h, wg_h, wu_h, wd_h, hist_h, slot, lens_h, kc_h, vc_h, spread_h,
    att_o, q_o, k_o, v_o, o_o, g_o, u_o, d_o, nh_o,
    wq, wk, wv, wo, wg, wu, wd, kc, vc, hid, hist, spread, lens, sent, got, fac,
    pk_s, pk_r, pt_s, pt_r, part, one_r, two_s, two_r,
    load_sem, send_sem, recv_sem, pks_sem, pkr_sem, pts_sem, ptr_sem,
    ones_sem, oner_sem, twos_sem, twor_sem, hop_sem,
    left_s, left_r, lfs_sem, lfr_sem,
):
    loads = [
        pltpu.make_async_copy(src, dst, load_sem.at[n])
        for n, (src, dst) in enumerate(
            [(wg_h, wg), (wq_h, wq), (wk_h, wk), (wv_h, wv), (wu_h, wu), (wd_h, wd), (wo_h, wo),
             (hid_h, hid), (hist_h, hist), (spread_h, spread), (lens_h, lens), (kc_h, kc), (vc_h, vc)]
        )
    ]
    for load in loads[:4]:
        load.start()

    me = lax.axis_index("fsdp")
    tp = lax.axis_index("tp")
    my_y, my_z, my_c = lax.div(me, 16), lax.rem(lax.div(me, 2), 8), lax.rem(me, 2)

    def device(dy, dz, dc):
        return lax.rem(my_y + dy, 2) * 16 + lax.rem(my_z + dz, 8) * 2 + lax.rem(my_c + dc, 2)

    def source(i):
        dy, dz, dc = offset(i)
        return device(dy, 8 - dz, dc)

    partners = [None] + [device(*offset(i)) for i in range(1, N)]
    near, middle, far = [*range(4, 12), *range(1, 4)], range(12, 20), range(20, N)

    barrier = pltpu.get_barrier_semaphore()
    for i in near:
        pl.semaphore_signal(barrier, 1, device_id={"fsdp": partners[i]}, device_id_type=MESH)
    for i in range(1, TP):
        pl.semaphore_signal(barrier, 1, device_id={"tp": lax.rem(tp + i, TP)}, device_id_type=MESH)

    shift = lax.rem(WIDE * me, LANES)

    def pack(tile, parts, chunk_of=lambda i: i, count=D // CHUNK):
        def body(i, _):
            cols = pl.ds(pl.multiple_of(chunk_of(i) * CHUNK, CHUNK), CHUNK)
            pieces = [ref[lo:hi, cols].astype(F32) for ref, lo, hi in parts]
            rows = sum(hi - lo for _, lo, hi in parts)
            if rows < LANES:
                pieces.append(jnp.zeros((LANES - rows, CHUNK), F32))
            block = jnp.concatenate(pieces, axis=0).T
            sent[tile, cols, :] = pltpu.roll(block, shift, 1).astype(BF16)
            return 0

        lax.fori_loop(0, count, body, 0)

    lane = lax.broadcasted_iota(jnp.int32, (1, LANES), 1)

    own_lanes = lax.div(lax.broadcasted_iota(jnp.int32, (TAIL, LANES), 1), REST) == lax.broadcasted_iota(
        jnp.int32, (TAIL, LANES), 0
    )

    tail_row = lax.broadcasted_iota(jnp.int32, (TAIL, LANES), 0)

    def slant(x, step):
        for bit in (1, 2, 4, 8):
            x = jnp.where(lax.rem(lax.div(tail_row, bit), 2) == 1, pltpu.roll(x, step * bit % LANES, 1), x)
        return x

    def fold(d, _):
        first = pl.multiple_of(d * ROWS, ROWS)
        tail = sent[1, pl.ds(pl.multiple_of(first + SENT, TAIL), TAIL), :].astype(F32)
        moved = jnp.concatenate([pltpu.roll(tail, WIDE + REST - SPARE * k, 1) for k in range(MOVES)], axis=0)
        free = lax.rem(lane - shift + LANES, LANES) >= WIDE + REST
        rows = pl.ds(first, SENT)
        sent[1, rows, :] = jnp.where(free, moved, sent[1, rows, :].astype(F32)).astype(BF16)
        turned = slant(pltpu.roll(tail, lax.rem(2 * LANES - WIDE - shift, LANES), 1), REST)
        left_s[d] = jnp.sum(jnp.where(own_lanes, turned, 0.0), axis=0, keepdims=True)
        return 0

    def unfold(block, left, s):
        x = block.astype(F32)
        base = lax.rem(WIDE * s, LANES)
        at = lax.rem(lane - base + LANES, LANES)
        spread_out = jnp.where(own_lanes, jnp.broadcast_to(left, (TAIL, LANES)), 0.0)
        tail = pltpu.roll(slant(spread_out, LANES - REST), lax.rem(WIDE + base, LANES), 1)
        for k in range(MOVES):
            piece = pltpu.roll(x[TAIL * k : TAIL * (k + 1), :], SPARE * (k + 1), 1)
            tail = jnp.where((at >= SPARE * k) & (at < SPARE * (k + 1)), piece, tail)
        return jnp.concatenate([x, tail], axis=0)

    def left_copy(to, slot_of, j=0):
        return pltpu.make_async_remote_copy(
            left_s.at[to], left_r.at[slot_of], lfs_sem.at[j], lfr_sem.at[slot_of], device_id={"fsdp": to}, device_id_type=MESH
        )

    def block_copy(tile, to, slot_of, j=0):
        return pltpu.make_async_remote_copy(
            sent.at[tile, pl.ds(pl.multiple_of(to * ROWS, ROWS), SENT if tile == 1 else ROWS)],
            got.at[tile, slot_of, pl.ds(0, SENT if tile == 1 else ROWS)],
            send_sem.at[tile, j],
            recv_sem.at[tile, slot_of],
            device_id={"fsdp": to},
            device_id_type=MESH,
        )

    def send(tile, order=range(N - 1, 0, -1)):
        for i in order:
            block_copy(tile, partners[i], me, i).start()

    for n in range(4):
        loads[n].wait()
    for load in loads[4:11]:
        load.start()
    first_tile = [(wg, 0, HEAD_COLS), (wq, 0, SLIM), (wk, 0, TINY), (wv, 0, TINY)]
    pair = lax.div(my_z, 2)
    beside = lax.rem(pair + 3 + 2 * lax.rem(my_z, 2), 4)

    def near_chunk(i):
        return lax.rem(i, 2) * 4 + pair + lax.div(i, 2) * (beside - pair)

    def far_chunk(i):
        return lax.rem(i, 2) * 4 + lax.rem(pair + lax.div(i, 2) * (beside - pair) + 2, 4)

    pack(0, first_tile, near_chunk, 4)
    pl.semaphore_wait(barrier, len(near) + TP - 1)

    def peak_copy(to, slot_of, j=0):
        return pltpu.make_async_remote_copy(
            pk_s, pk_r.at[slot_of], pks_sem.at[j], pkr_sem.at[slot_of], device_id={"fsdp": to}, device_id_type=MESH
        )

    def relay(sem, dz):
        for step in (dz, 8 - dz):
            pl.semaphore_signal(sem, 1, device_id={"fsdp": device(0, step, 0)}, device_id_type=MESH)

    relay(hop_sem.at[0], 1)
    send(0, near)

    for n in range(4, 7):
        loads[n].wait()

    mine = jnp.zeros((1, LANES), F32)
    for t, ref in enumerate((wq, wk, wv, wo, wg, wu, wd)):
        def body(c, best, ref=ref):
            cols = pl.ds(pl.multiple_of(c * CHUNK, CHUNK), CHUNK)
            return jnp.maximum(best, jnp.max(jnp.abs(ref[:, cols].astype(F32)), axis=0, keepdims=True))

        best = lax.fori_loop(0, D // CHUNK, body, jnp.zeros((1, CHUNK), F32))
        mine = jnp.where(lane == t, jnp.max(best, axis=1, keepdims=True), mine)
    pk_s[...] = mine

    def send_peaks(order):
        for i in order:
            peak_copy(partners[i], me, i).start()

    send_peaks(near)
    pack(0, first_tile, far_chunk, 4)
    pl.semaphore_wait(hop_sem.at[0], 2)
    relay(hop_sem.at[1], 2)
    send_peaks(middle)
    send(0, middle)
    pl.semaphore_wait(hop_sem.at[1], 2)
    send_peaks(far)
    send(0, far)
    for load in loads[11:]:
        load.start()
    pack(1, [(wu, 0, WIDE), (wg, HEAD_COLS, WIDE)])
    lax.fori_loop(0, N, fold, 0)
    for i in range(N - 1, 0, -1):
        left_copy(partners[i], me, i).start()
    send(1)

    def wait_peak(i, best):
        src = source(i)
        peak_copy(src, src).wait_recv()
        return jnp.maximum(best, pk_r[src])

    pt_s[...] = lax.fori_loop(1, N, wait_peak, mine)

    def tp_copy(to, slot_of, i=0):
        return pltpu.make_async_remote_copy(
            pt_s, pt_r.at[slot_of], pts_sem.at[i], ptr_sem.at[slot_of], device_id={"tp": to}, device_id_type=MESH
        )

    for i in range(1, TP):
        tp_copy(lax.rem(tp + i, TP), tp, i).start()
    pack(2, [(wd, 0, WIDE), (wo, 0, SLIM)])

    def wait_tp(i, best):
        src = lax.rem(tp + TP - i, TP)
        tp_copy(src, src).wait_recv()
        return jnp.maximum(best, pt_r[src])

    peaks = lax.fori_loop(1, TP, wait_tp, pt_s[...])

    for n in range(7, 11):
        loads[n].wait()
    on_row = lax.broadcasted_iota(jnp.int32, (7, LANES), 0) == lax.broadcasted_iota(jnp.int32, (7, LANES), 1)
    peaks_column = jnp.sum(jnp.where(on_row, peaks, 0.0), axis=1, keepdims=True)
    marked = lax.broadcasted_iota(jnp.int32, (7, HIST), 1) == slot[0]
    past = hist[...]
    kept = jnp.max(jnp.where(marked, 0.0, past), axis=1, keepdims=True)
    nh_o[...] = jnp.where(marked, peaks_column, past)
    fac[0:7, :] = jnp.broadcast_to(target_peak / jnp.maximum(peaks_column, kept), (7, LANES))

    def put(ref, tile, mask, value):
        cols = pl.ds(pl.multiple_of(tile * LANES, LANES), LANES)
        ref[:, cols] = jnp.where(mask, value, ref[:, cols].astype(F32)).astype(BF16)

    def place(ref, first, count, value):
        tiles = ref.shape[1] // LANES
        tile, at = lax.div(first, LANES), lax.rem(first, LANES)
        put(ref, tile, (lane >= at) & (lane < at + count), value)
        if tiles > 1:
            put(ref, tile + 1 - lax.div(tile + 1, tiles), lane < at + count - LANES, value)

    def turn(value, now, then):
        return pltpu.roll(value, lax.rem(then - now + 4 * LANES, LANES), 1)

    def process(tile, block, s):
        x = block.astype(F32)
        base = lax.rem(WIDE * s, LANES)
        if tile == 0:
            place(g_o, WIDE * s, HEAD_COLS, x * fac[4:5, :])
            place(q_o, SLIM * s, SLIM, turn(x * fac[0:1, :], base + HEAD_COLS, lax.rem(SLIM * s, LANES)))
            place(k_o, TINY * s, TINY, turn(x * fac[1:2, :], base + HEAD_COLS + SLIM, TINY * s))
            place(v_o, TINY * s, TINY, turn(x * fac[2:3, :], base + HEAD_COLS + SLIM + TINY, TINY * s))
        elif tile == 1:
            place(u_o, WIDE * s, WIDE, x * fac[5:6, :])
            place(g_o, WIDE * s + HEAD_COLS, REST, turn(x * fac[4:5, :], base + WIDE, lax.rem(WIDE * s + HEAD_COLS, LANES)))
        else:
            place(d_o, WIDE * s, WIDE, x * fac[6:7, :])
            place(o_o, SLIM * s, SLIM, turn(x * fac[3:4, :], base + WIDE, lax.rem(SLIM * s, LANES)))

    def receive(tile):
        process(tile, sent[tile, pl.ds(pl.multiple_of(me * ROWS, ROWS), ROWS), :], me)

        def body(j, _):
            src = source(1 + j if tile == 0 else N - 1 - j)
            block_copy(tile, src, src).wait_recv()
            if tile == 1:
                left_copy(src, src).wait_recv()
                process(tile, unfold(got[1, src, 0:SENT, :], left_r[src], src), src)
            else:
                process(tile, got[tile, src], src)
            return 0

        lax.fori_loop(0, N - 1, body, 0)

    receive(0)

    row = lax.broadcasted_iota(jnp.int32, (64, 64), 0)
    col = lax.broadcasted_iota(jnp.int32, (64, 64), 1)
    owner = (row // 32) * 32 + ((row // 2) % 8) * 4 + ((row // 16) % 2) * 2 + row % 2
    ordered = jnp.dot((owner == col).astype(BF16), hid[...], preferred_element_type=F32)
    hidden = ordered.astype(BF16)
    part[:, 0:640] = jnp.dot(hidden, q_o[...], preferred_element_type=F32)
    part[:, 640:768] = jnp.dot(hidden, k_o[...], preferred_element_type=F32)
    part[:, 768:896] = jnp.dot(hidden, v_o[...], preferred_element_type=F32)
    part[:, 896:1024] = jnp.broadcast_to(jnp.sum(ordered * ordered, axis=1, keepdims=True), (64, LANES))

    group = my_y * 2 + my_c

    def one_copy(k, receiving):
        y, c = lax.rem(my_y + k // 2, 2), lax.rem(my_c + k % 2, 2)
        other = y * 2 + c
        return other, pltpu.make_async_remote_copy(
            part.at[pl.ds(pl.multiple_of(other * 16, 16), 16)],
            one_r.at[other if receiving else group],
            ones_sem.at[other],
            oner_sem.at[other if receiving else group],
            device_id={"fsdp": y * 16 + my_z * 2 + c},
            device_id_type=MESH,
        )

    for k in range(1, 4):
        one_copy(k, False)[1].start()
    total = part[pl.ds(pl.multiple_of(group * 16, 16), 16), :]
    for k in range(1, 4):
        other, copy = one_copy(k, True)
        copy.wait_recv()
        total = total + one_r[other]
    for z in range(8):
        two_s[z] = total[2 * z : 2 * z + 2, :]

    def two_copy(z, slot_of, i=0):
        return pltpu.make_async_remote_copy(
            two_s.at[z],
            two_r.at[slot_of],
            twos_sem.at[i],
            twor_sem.at[slot_of],
            device_id={"fsdp": my_y * 16 + z * 2 + my_c},
            device_id_type=MESH,
        )

    for i in range(1, 8):
        two_copy(lax.rem(my_z + i, 8), my_z, i).start()
    send(2)
    receive(1)

    def wait_two(i, total):
        src = lax.rem(my_z + 8 - i, 8)
        two_copy(src, src).wait_recv()
        return total + two_r[src]

    summed = lax.fori_loop(1, 8, wait_two, two_s[my_z])

    inv_rms = lax.rsqrt(summed[:, 896:1024] / D + norm_eps)
    token = lax.broadcasted_iota(jnp.int32, (2, LANES), 0)
    length = jnp.where(token == 0, lens[0], lens[1])
    angle = length.astype(F32) * spread[...]
    half = lax.broadcasted_iota(jnp.int32, (2, LANES), 1) < HEAD_DIM // 2
    cosine = jnp.cos(angle)
    sine = jnp.where(half, -jnp.sin(angle), jnp.sin(angle))

    def rotate(x):
        return x * cosine + pltpu.roll(x, HEAD_DIM // 2, 1) * sine

    heads = [
        rotate(summed[:, h * LANES : (h + 1) * LANES] * inv_rms / fac[0:1, :]).astype(BF16).astype(F32)
        for h in range(GROUP)
    ]
    key_new = rotate(summed[:, 640:768] * inv_rms / fac[1:2, :]).astype(BF16).astype(F32)
    value_new = (summed[:, 768:896] * inv_rms / fac[2:3, :]).astype(BF16).astype(F32)
    loads[11].wait()
    loads[12].wait()
    head_row = lax.broadcasted_iota(jnp.int32, (8, LANES), 0)
    scale = HEAD_DIM ** (-0.5)
    mixes = []
    for b in range(2):
        query = jnp.zeros((8, LANES), F32)
        for h in range(GROUP):
            query = jnp.where(head_row == h, heads[h][b : b + 1, :], query)
        scores = (
            lax.dot_general(query.astype(BF16), kc[b], (((1,), (1,)), ((), ())), preferred_element_type=F32) * scale
        )
        own = jnp.sum(query * key_new[b : b + 1, :], axis=1, keepdims=True) * scale
        valid = lax.broadcasted_iota(jnp.int32, (8, CACHE), 1) < lens[b]
        top = jnp.maximum(jnp.max(jnp.where(valid, scores, -1e30), axis=1, keepdims=True), own)
        weights = jnp.where(valid, jnp.exp(scores - top), 0.0)
        own_weight = jnp.exp(own - top)
        total = jnp.sum(weights, axis=1, keepdims=True) + own_weight
        probs = (weights / total).astype(BF16)
        own_prob = (own_weight / total).astype(BF16).astype(F32)
        mixed = jnp.dot(probs, vc[b], preferred_element_type=F32)
        mixes.append(mixed + own_prob * value_new[b : b + 1, :])
    for h in range(GROUP):
        pair = jnp.where(token == 0, mixes[0][h : h + 1, :], mixes[1][h : h + 1, :])
        att_o[:, h * LANES : (h + 1) * LANES] = pair.astype(BF16)

    for i in range(1, N):
        peak_copy(partners[i], me, i).wait_send()
        left_copy(partners[i], me, i).wait_send()
        for tile in range(2):
            block_copy(tile, partners[i], me, i).wait_send()
    for i in range(1, TP):
        tp_copy(lax.rem(tp + i, TP), tp, i).wait_send()
    for k in range(1, 4):
        one_copy(k, False)[1].wait_send()
    for i in range(1, 8):
        two_copy(lax.rem(my_z + i, 8), my_z, i).wait_send()
    receive(2)
    for i in range(1, N):
        block_copy(2, partners[i], me, i).wait_send()


def finish(*refs):
    count = (len(refs) - 1) // 2
    copies = [pltpu.make_async_copy(refs[n], refs[count + n], refs[-1].at[n]) for n in range(count)]
    for copy in copies:
        copy.start()
    for copy in copies:
        copy.wait()


def per_device(
    hidden, query_weight, key_weight, value_weight, output_weight, gate_weight, up_weight, down_weight,
    history, slot, lengths, key_cache, value_cache,
):
    spread = np.float64(rope_theta) ** (-2.0 * (np.arange(HEAD_DIM) % (HEAD_DIM // 2)) / HEAD_DIM)
    spread = jnp.asarray(spread.astype(np.float32)[None, :])
    vmem = pl.BlockSpec(memory_space=pltpu.VMEM)
    hbm = pl.BlockSpec(memory_space=pltpu.HBM)
    out = [
        ((2, GROUP * HEAD_DIM), BF16),
        ((ROWS, 640), BF16),
        ((ROWS, 128), BF16),
        ((ROWS, 128), BF16),
        ((ROWS, 640), BF16),
        ((ROWS, 3456), BF16),
        ((ROWS, 3456), BF16),
        ((ROWS, 3456), BF16),
        ((7, HIST), F32),
    ]
    dma = pltpu.SemaphoreType.DMA
    results = pl.pallas_call(
        kernel,
        out_shape=[pltpu.VMEM(s, t) for s, t in out],
        in_specs=[hbm] * 9 + [pl.BlockSpec(memory_space=pltpu.SMEM)] + [hbm] * 4,
        out_specs=[vmem] * 9,
        scratch_shapes=[
            pltpu.VMEM((SLIM, D), BF16),
            pltpu.VMEM((TINY, D), BF16),
            pltpu.VMEM((TINY, D), BF16),
            pltpu.VMEM((SLIM, D), BF16),
            pltpu.VMEM((WIDE, D), BF16),
            pltpu.VMEM((WIDE, D), BF16),
            pltpu.VMEM((WIDE, D), BF16),
            pltpu.VMEM((2, CACHE, HEAD_DIM), BF16),
            pltpu.VMEM((2, CACHE, HEAD_DIM), BF16),
            pltpu.VMEM((64, ROWS), BF16),
            pltpu.VMEM((7, HIST), F32),
            pltpu.VMEM((1, LANES), F32),
            pltpu.SMEM((2,), jnp.int32),
            pltpu.VMEM((3, D, LANES), BF16),
            pltpu.VMEM((3, N, ROWS, LANES), BF16),
            pltpu.VMEM((8, LANES), F32),
            pltpu.VMEM((1, LANES), F32),
            pltpu.VMEM((N, 1, LANES), F32),
            pltpu.VMEM((1, LANES), F32),
            pltpu.VMEM((TP, 1, LANES), F32),
            pltpu.VMEM((64, 1024), F32),
            pltpu.VMEM((4, 16, 1024), F32),
            pltpu.VMEM((8, 2, 1024), F32),
            pltpu.VMEM((8, 2, 1024), F32),
            dma((13,)),
            dma((3, N)),
            dma((3, N)),
            dma((N,)),
            dma((N,)),
            dma((TP,)),
            dma((TP,)),
            dma((4,)),
            dma((4,)),
            dma((8,)),
            dma((8,)),
            pltpu.SemaphoreType.REGULAR((2,)),
            pltpu.VMEM((N, 1, LANES), F32),
            pltpu.VMEM((N, 1, LANES), F32),
            dma((N,)),
            dma((N,)),
        ],
        compiler_params=pltpu.CompilerParams(
            collective_id=0, has_side_effects=True, vmem_limit_bytes=VMEM_LIMIT
        ),
    )(
        *(
            x if x is slot else pltpu.with_memory_space_constraint(x, pltpu.HBM)
            for x in (
                hidden, query_weight.T, key_weight.T, value_weight.T, output_weight, gate_weight.T, up_weight.T,
                down_weight, history, slot, lengths, key_cache, value_cache, spread,
            )
        )
    )
    results = pl.pallas_call(
        finish,
        out_shape=[jax.ShapeDtypeStruct(s, t) for s, t in out],
        in_specs=[vmem] * 9,
        out_specs=[hbm] * 9,
        scratch_shapes=[dma((9,))],
        compiler_params=pltpu.CompilerParams(vmem_limit_bytes=8 * 2**20),
    )(*results)
    attention_out, query, key, value, output, gate, up, down, new_history = results
    return attention_out, query, key, value, output.T, gate, up, down.T, new_history


def solution(mesh):
    f, t = "fsdp", "tp"
    in_specs = (
        P(None, f), P(None, (t, f)), P(None, (t, f)), P(None, (t, f)), P((t, f), None), P(None, (t, f)),
        P(None, (t, f)), P((t, f), None), P(), P(), P(f), P(f, None, t), P(f, None, t),
    )
    out_specs = (P(f, t), P(f, t), P(f, t), P(f, t), P(t, f), P(f, t), P(f, t), P(t, f), P())
    return jax.shard_map(per_device, mesh=mesh, in_specs=in_specs, out_specs=out_specs, check_vma=False)
```

```python
import functools
import math

import jax
import jax.numpy as jnp
import numpy as np
from jax import lax
from jax.experimental import pallas as pl
from jax.experimental.pallas import tpu as pltpu
from jax.sharding import PartitionSpec as P

D = 5120
HEADS = 40
KV_HEADS = 8
HEAD_DIM = 128
GROUP = HEADS // KV_HEADS
CACHE = 4096
HIST = 1024
N = 32
TP = 8
ROWS = D // N
WIDE = 27648 // (N * TP)
SLIM = D // (N * TP)
TINY = KV_HEADS * HEAD_DIM // (N * TP)
LANES = 128
HEAD_COLS = LANES - SLIM - 2 * TINY
REST = WIDE - HEAD_COLS
CHUNK = 640
SPARE = LANES - WIDE - REST
TAIL = 16
SENT = ROWS - TAIL
MOVES = WIDE // SPARE
VMEM_LIMIT = 40 * 2**20

target_peak = 4.0
norm_eps = 1e-06
rope_theta = 1000000.0

F32 = jnp.float32
BF16 = jnp.bfloat16
MESH = pl.DeviceIdType.MESH


def offset(i):
    k = lax.div(i, 4) if isinstance(i, jax.Array) else i // 4
    odd = lax.rem(k, 2) if isinstance(i, jax.Array) else k % 2
    if isinstance(i, jax.Array):
        return lax.rem(lax.div(i, 2), 2), lax.rem(lax.div(k + 1, 2) * (2 * odd - 1) + 8, 8), lax.rem(i, 2)
    return (i // 2) % 2, ((k + 1) // 2 * (2 * odd - 1)) % 8, i % 2


def kernel(
    hid_h, wq_h, wk_h, wv_h, wo_h, wg_h, wu_h, wd_h, hist_h, slot, lens_h, kc_h, vc_h, spread_h,
    att_o, q_o, k_o, v_o, o_o, g_o, u_o, d_o, nh_o,
    wq, wk, wv, wo, wg, wu, wd, kc, vc, hid, hist, spread, lens, sent, got, fac,
    pk_s, pk_r, pt_s, pt_r, part, one_r, two_s, two_r,
    load_sem, send_sem, recv_sem, pks_sem, pkr_sem, pts_sem, ptr_sem,
    ones_sem, oner_sem, twos_sem, twor_sem, hop_sem,
    left_s, left_r, lfs_sem, lfr_sem,
):
    loads = [
        pltpu.make_async_copy(src, dst, load_sem.at[n])
        for n, (src, dst) in enumerate(
            [(wg_h, wg), (wq_h, wq), (wk_h, wk), (wv_h, wv), (wu_h, wu), (wd_h, wd), (wo_h, wo),
             (hid_h, hid), (hist_h, hist), (spread_h, spread), (lens_h, lens), (kc_h, kc), (vc_h, vc)]
        )
    ]
    for load in loads[:4]:
        load.start()

    me = lax.axis_index("fsdp")
    tp = lax.axis_index("tp")
    my_y, my_z, my_c = lax.div(me, 16), lax.rem(lax.div(me, 2), 8), lax.rem(me, 2)

    def device(dy, dz, dc):
        return lax.rem(my_y + dy, 2) * 16 + lax.rem(my_z + dz, 8) * 2 + lax.rem(my_c + dc, 2)

    def source(i):
        dy, dz, dc = offset(i)
        return device(dy, 8 - dz, dc)

    partners = [None] + [device(*offset(i)) for i in range(1, N)]
    near, middle, far = [*range(4, 12), *range(1, 4)], range(12, 20), range(20, N)

    barrier = pltpu.get_barrier_semaphore()
    for i in near:
        pl.semaphore_signal(barrier, 1, device_id={"fsdp": partners[i]}, device_id_type=MESH)
    for i in range(1, TP):
        pl.semaphore_signal(barrier, 1, device_id={"tp": lax.rem(tp + i, TP)}, device_id_type=MESH)

    shift = lax.rem(WIDE * me, LANES)

    def pack(tile, parts, chunk_of=lambda i: i, count=D // CHUNK):
        def body(i, _):
            cols = pl.ds(pl.multiple_of(chunk_of(i) * CHUNK, CHUNK), CHUNK)
            pieces = [ref[lo:hi, cols].astype(F32) for ref, lo, hi in parts]
            rows = sum(hi - lo for _, lo, hi in parts)
            if rows < LANES:
                pieces.append(jnp.zeros((LANES - rows, CHUNK), F32))
            block = jnp.concatenate(pieces, axis=0).T
            sent[tile, cols, :] = pltpu.roll(block, shift, 1).astype(BF16)
            return 0

        lax.fori_loop(0, count, body, 0)

    lane = lax.broadcasted_iota(jnp.int32, (1, LANES), 1)

    own_lanes = lax.div(lax.broadcasted_iota(jnp.int32, (TAIL, LANES), 1), REST) == lax.broadcasted_iota(
        jnp.int32, (TAIL, LANES), 0
    )

    tail_row = lax.broadcasted_iota(jnp.int32, (TAIL, LANES), 0)

    def slant(x, step):
        for bit in (1, 2, 4, 8):
            x = jnp.where(lax.rem(lax.div(tail_row, bit), 2) == 1, pltpu.roll(x, step * bit % LANES, 1), x)
        return x

    def fold(d, _):
        first = pl.multiple_of(d * ROWS, ROWS)
        tail = sent[1, pl.ds(pl.multiple_of(first + SENT, TAIL), TAIL), :].astype(F32)
        moved = jnp.concatenate([pltpu.roll(tail, WIDE + REST - SPARE * k, 1) for k in range(MOVES)], axis=0)
        free = lax.rem(lane - shift + LANES, LANES) >= WIDE + REST
        rows = pl.ds(first, SENT)
        sent[1, rows, :] = jnp.where(free, moved, sent[1, rows, :].astype(F32)).astype(BF16)
        turned = slant(pltpu.roll(tail, lax.rem(2 * LANES - WIDE - shift, LANES), 1), REST)
        left_s[d] = jnp.sum(jnp.where(own_lanes, turned, 0.0), axis=0, keepdims=True)
        return 0

    def unfold(block, left, s):
        x = block.astype(F32)
        base = lax.rem(WIDE * s, LANES)
        at = lax.rem(lane - base + LANES, LANES)
        spread_out = jnp.where(own_lanes, jnp.broadcast_to(left, (TAIL, LANES)), 0.0)
        tail = pltpu.roll(slant(spread_out, LANES - REST), lax.rem(WIDE + base, LANES), 1)
        for k in range(MOVES):
            piece = pltpu.roll(x[TAIL * k : TAIL * (k + 1), :], SPARE * (k + 1), 1)
            tail = jnp.where((at >= SPARE * k) & (at < SPARE * (k + 1)), piece, tail)
        return jnp.concatenate([x, tail], axis=0)

    def left_copy(to, slot_of, j=0):
        return pltpu.make_async_remote_copy(
            left_s.at[to], left_r.at[slot_of], lfs_sem.at[j], lfr_sem.at[slot_of], device_id={"fsdp": to}, device_id_type=MESH
        )

    def block_copy(tile, to, slot_of, j=0):
        return pltpu.make_async_remote_copy(
            sent.at[tile, pl.ds(pl.multiple_of(to * ROWS, ROWS), SENT if tile == 1 else ROWS)],
            got.at[tile, slot_of, pl.ds(0, SENT if tile == 1 else ROWS)],
            send_sem.at[tile, j],
            recv_sem.at[tile, slot_of],
            device_id={"fsdp": to},
            device_id_type=MESH,
        )

    def send(tile, order=range(N - 1, 0, -1)):
        for i in order:
            block_copy(tile, partners[i], me, i).start()

    for n in range(4):
        loads[n].wait()
    for load in loads[4:11]:
        load.start()
    first_tile = [(wg, 0, HEAD_COLS), (wq, 0, SLIM), (wk, 0, TINY), (wv, 0, TINY)]
    pair = lax.div(my_z, 2)
    beside = lax.rem(pair + 3 + 2 * lax.rem(my_z, 2), 4)

    def near_chunk(i):
        return lax.rem(i, 2) * 4 + pair + lax.div(i, 2) * (beside - pair)

    def far_chunk(i):
        return lax.rem(i, 2) * 4 + lax.rem(pair + lax.div(i, 2) * (beside - pair) + 2, 4)

    pack(0, first_tile, near_chunk, 4)
    pl.semaphore_wait(barrier, len(near) + TP - 1)

    def peak_copy(to, slot_of, j=0):
        return pltpu.make_async_remote_copy(
            pk_s, pk_r.at[slot_of], pks_sem.at[j], pkr_sem.at[slot_of], device_id={"fsdp": to}, device_id_type=MESH
        )

    def relay(sem, dz):
        for step in (dz, 8 - dz):
            pl.semaphore_signal(sem, 1, device_id={"fsdp": device(0, step, 0)}, device_id_type=MESH)

    relay(hop_sem.at[0], 1)
    send(0, near)

    for n in range(4, 7):
        loads[n].wait()

    mine = jnp.zeros((1, LANES), F32)
    for t, ref in enumerate((wq, wk, wv, wo, wg, wu, wd)):
        def body(c, best, ref=ref):
            cols = pl.ds(pl.multiple_of(c * CHUNK, CHUNK), CHUNK)
            return jnp.maximum(best, jnp.max(jnp.abs(ref[:, cols].astype(F32)), axis=0, keepdims=True))

        best = lax.fori_loop(0, D // CHUNK, body, jnp.zeros((1, CHUNK), F32))
        mine = jnp.where(lane == t, jnp.max(best, axis=1, keepdims=True), mine)
    loads[7].wait()
    features = hid[...].astype(F32)
    squares = jnp.sum(features * features, axis=1, keepdims=True)
    on_lane = lax.broadcasted_iota(jnp.int32, (64, LANES), 0) + 64 == lax.broadcasted_iota(jnp.int32, (64, LANES), 1)
    mine = jnp.where(lane >= 64, jnp.sum(jnp.where(on_lane, squares, 0.0), axis=0, keepdims=True), mine)
    pk_s[...] = mine

    def send_peaks(order):
        for i in order:
            peak_copy(partners[i], me, i).start()

    send_peaks(near)
    pack(0, first_tile, far_chunk, 4)
    pl.semaphore_wait(hop_sem.at[0], 2)
    relay(hop_sem.at[1], 2)
    send_peaks(middle)
    send(0, middle)
    pl.semaphore_wait(hop_sem.at[1], 2)
    send_peaks(far)
    send(0, far)
    for load in loads[11:]:
        load.start()
    pack(1, [(wu, 0, WIDE), (wg, HEAD_COLS, WIDE)])
    lax.fori_loop(0, N, fold, 0)
    for i in range(N - 1, 0, -1):
        left_copy(partners[i], me, i).start()
    send(1)

    def wait_peak(i, best):
        src = source(i)
        peak_copy(src, src).wait_recv()
        return jnp.where(lane >= 64, best + pk_r[src], jnp.maximum(best, pk_r[src]))

    over_fsdp = lax.fori_loop(1, N, wait_peak, mine)
    pt_s[...] = over_fsdp

    def tp_copy(to, slot_of, i=0):
        return pltpu.make_async_remote_copy(
            pt_s, pt_r.at[slot_of], pts_sem.at[i], ptr_sem.at[slot_of], device_id={"tp": to}, device_id_type=MESH
        )

    for i in range(1, TP):
        tp_copy(lax.rem(tp + i, TP), tp, i).start()
    pack(2, [(wd, 0, WIDE), (wo, 0, SLIM)])

    def wait_tp(i, best):
        src = lax.rem(tp + TP - i, TP)
        tp_copy(src, src).wait_recv()
        return jnp.maximum(best, pt_r[src])

    peaks = lax.fori_loop(1, TP, wait_tp, pt_s[...])

    for n in range(8, 11):
        loads[n].wait()
    on_row = lax.broadcasted_iota(jnp.int32, (7, LANES), 0) == lax.broadcasted_iota(jnp.int32, (7, LANES), 1)
    peaks_column = jnp.sum(jnp.where(on_row, peaks, 0.0), axis=1, keepdims=True)
    marked = lax.broadcasted_iota(jnp.int32, (7, HIST), 1) == slot[0]
    past = hist[...]
    kept = jnp.max(jnp.where(marked, 0.0, past), axis=1, keepdims=True)
    nh_o[...] = jnp.where(marked, peaks_column, past)
    fac[0:7, :] = jnp.broadcast_to(target_peak / jnp.maximum(peaks_column, kept), (7, LANES))

    def put(ref, tile, mask, value):
        cols = pl.ds(pl.multiple_of(tile * LANES, LANES), LANES)
        ref[:, cols] = jnp.where(mask, value, ref[:, cols].astype(F32)).astype(BF16)

    def place(ref, first, count, value):
        tiles = ref.shape[1] // LANES
        tile, at = lax.div(first, LANES), lax.rem(first, LANES)
        put(ref, tile, (lane >= at) & (lane < at + count), value)
        if tiles > 1:
            put(ref, tile + 1 - lax.div(tile + 1, tiles), lane < at + count - LANES, value)

    def turn(value, now, then):
        return pltpu.roll(value, lax.rem(then - now + 4 * LANES, LANES), 1)

    def process(tile, block, s):
        x = block.astype(F32)
        base = lax.rem(WIDE * s, LANES)
        if tile == 0:
            place(g_o, WIDE * s, HEAD_COLS, x * fac[4:5, :])
            place(q_o, SLIM * s, SLIM, turn(x * fac[0:1, :], base + HEAD_COLS, lax.rem(SLIM * s, LANES)))
            place(k_o, TINY * s, TINY, turn(x * fac[1:2, :], base + HEAD_COLS + SLIM, TINY * s))
            place(v_o, TINY * s, TINY, turn(x * fac[2:3, :], base + HEAD_COLS + SLIM + TINY, TINY * s))
        elif tile == 1:
            place(u_o, WIDE * s, WIDE, x * fac[5:6, :])
            place(g_o, WIDE * s + HEAD_COLS, REST, turn(x * fac[4:5, :], base + WIDE, lax.rem(WIDE * s + HEAD_COLS, LANES)))
        else:
            place(d_o, WIDE * s, WIDE, x * fac[6:7, :])
            place(o_o, SLIM * s, SLIM, turn(x * fac[3:4, :], base + WIDE, lax.rem(SLIM * s, LANES)))

    def receive(tile):
        process(tile, sent[tile, pl.ds(pl.multiple_of(me * ROWS, ROWS), ROWS), :], me)

        def body(j, _):
            src = source(1 + j if tile == 0 else N - 1 - j)
            block_copy(tile, src, src).wait_recv()
            if tile == 1:
                left_copy(src, src).wait_recv()
                process(tile, unfold(got[1, src, 0:SENT, :], left_r[src], src), src)
            else:
                process(tile, got[tile, src], src)
            return 0

        lax.fori_loop(0, N - 1, body, 0)

    receive(0)

    row = lax.broadcasted_iota(jnp.int32, (64, 64), 0)
    col = lax.broadcasted_iota(jnp.int32, (64, 64), 1)
    owner = (row // 32) * 32 + ((row // 2) % 8) * 4 + ((row // 16) % 2) * 2 + row % 2
    ordered = jnp.dot((owner == col).astype(BF16), hid[...], preferred_element_type=F32)
    hidden = ordered.astype(BF16)
    part[:, 0:640] = jnp.dot(hidden, q_o[...], preferred_element_type=F32)
    part[:, 640:768] = jnp.dot(hidden, k_o[...], preferred_element_type=F32)
    part[:, 768:896] = jnp.dot(hidden, v_o[...], preferred_element_type=F32)

    group = my_y * 2 + my_c

    def one_copy(k, receiving):
        y, c = lax.rem(my_y + k // 2, 2), lax.rem(my_c + k % 2, 2)
        other = y * 2 + c
        return other, pltpu.make_async_remote_copy(
            part.at[pl.ds(pl.multiple_of(other * 16, 16), 16)],
            one_r.at[other if receiving else group],
            ones_sem.at[other],
            oner_sem.at[other if receiving else group],
            device_id={"fsdp": y * 16 + my_z * 2 + c},
            device_id_type=MESH,
        )

    for k in range(1, 4):
        one_copy(k, False)[1].start()
    total = part[pl.ds(pl.multiple_of(group * 16, 16), 16), :]
    for k in range(1, 4):
        other, copy = one_copy(k, True)
        copy.wait_recv()
        total = total + one_r[other]
    for z in range(8):
        two_s[z] = total[2 * z : 2 * z + 2, :]

    def two_copy(z, slot_of, i=0):
        return pltpu.make_async_remote_copy(
            two_s.at[z],
            two_r.at[slot_of],
            twos_sem.at[i],
            twor_sem.at[slot_of],
            device_id={"fsdp": my_y * 16 + z * 2 + my_c},
            device_id_type=MESH,
        )

    for i in range(1, 8):
        two_copy(lax.rem(my_z + i, 8), my_z, i).start()
    send(2)
    receive(1)

    def wait_two(i, total):
        src = lax.rem(my_z + 8 - i, 8)
        two_copy(src, src).wait_recv()
        return total + two_r[src]

    summed = lax.fori_loop(1, 8, wait_two, two_s[my_z])

    token = lax.broadcasted_iota(jnp.int32, (2, LANES), 0)
    own_squares = jnp.where(lane == 64 + 2 * me + token, jnp.broadcast_to(over_fsdp, (2, LANES)), 0.0)
    inv_rms = lax.rsqrt(jnp.sum(own_squares, axis=1, keepdims=True) / D + norm_eps)
    length = jnp.where(token == 0, lens[0], lens[1])
    angle = length.astype(F32) * spread[...]
    half = lax.broadcasted_iota(jnp.int32, (2, LANES), 1) < HEAD_DIM // 2
    cosine = jnp.cos(angle)
    sine = jnp.where(half, -jnp.sin(angle), jnp.sin(angle))

    def rotate(x):
        return x * cosine + pltpu.roll(x, HEAD_DIM // 2, 1) * sine

    heads = [
        rotate(summed[:, h * LANES : (h + 1) * LANES] * inv_rms / fac[0:1, :]).astype(BF16).astype(F32)
        for h in range(GROUP)
    ]
    key_new = rotate(summed[:, 640:768] * inv_rms / fac[1:2, :]).astype(BF16).astype(F32)
    value_new = (summed[:, 768:896] * inv_rms / fac[2:3, :]).astype(BF16).astype(F32)
    loads[11].wait()
    loads[12].wait()
    head_row = lax.broadcasted_iota(jnp.int32, (8, LANES), 0)
    scale = HEAD_DIM ** (-0.5)
    mixes = []
    for b in range(2):
        query = jnp.zeros((8, LANES), F32)
        for h in range(GROUP):
            query = jnp.where(head_row == h, heads[h][b : b + 1, :], query)
        scores = (
            lax.dot_general(query.astype(BF16), kc[b], (((1,), (1,)), ((), ())), preferred_element_type=F32) * scale
        )
        own = jnp.sum(query * key_new[b : b + 1, :], axis=1, keepdims=True) * scale
        valid = lax.broadcasted_iota(jnp.int32, (8, CACHE), 1) < lens[b]
        top = jnp.maximum(jnp.max(jnp.where(valid, scores, -1e30), axis=1, keepdims=True), own)
        weights = jnp.where(valid, jnp.exp(scores - top), 0.0)
        own_weight = jnp.exp(own - top)
        total = jnp.sum(weights, axis=1, keepdims=True) + own_weight
        probs = (weights / total).astype(BF16)
        own_prob = (own_weight / total).astype(BF16).astype(F32)
        mixed = jnp.dot(probs, vc[b], preferred_element_type=F32)
        mixes.append(mixed + own_prob * value_new[b : b + 1, :])
    for h in range(GROUP):
        pair = jnp.where(token == 0, mixes[0][h : h + 1, :], mixes[1][h : h + 1, :])
        att_o[:, h * LANES : (h + 1) * LANES] = pair.astype(BF16)

    for i in range(1, N):
        peak_copy(partners[i], me, i).wait_send()
        left_copy(partners[i], me, i).wait_send()
        for tile in range(2):
            block_copy(tile, partners[i], me, i).wait_send()
    for i in range(1, TP):
        tp_copy(lax.rem(tp + i, TP), tp, i).wait_send()
    for k in range(1, 4):
        one_copy(k, False)[1].wait_send()
    for i in range(1, 8):
        two_copy(lax.rem(my_z + i, 8), my_z, i).wait_send()
    receive(2)
    for i in range(1, N):
        block_copy(2, partners[i], me, i).wait_send()


def finish(*refs):
    count = (len(refs) - 1) // 2
    copies = [pltpu.make_async_copy(refs[n], refs[count + n], refs[-1].at[n]) for n in range(count)]
    for copy in copies:
        copy.start()
    for copy in copies:
        copy.wait()


def per_device(
    hidden, query_weight, key_weight, value_weight, output_weight, gate_weight, up_weight, down_weight,
    history, slot, lengths, key_cache, value_cache,
):
    spread = np.float64(rope_theta) ** (-2.0 * (np.arange(HEAD_DIM) % (HEAD_DIM // 2)) / HEAD_DIM)
    spread = jnp.asarray(spread.astype(np.float32)[None, :])
    vmem = pl.BlockSpec(memory_space=pltpu.VMEM)
    hbm = pl.BlockSpec(memory_space=pltpu.HBM)
    out = [
        ((2, GROUP * HEAD_DIM), BF16),
        ((ROWS, 640), BF16),
        ((ROWS, 128), BF16),
        ((ROWS, 128), BF16),
        ((ROWS, 640), BF16),
        ((ROWS, 3456), BF16),
        ((ROWS, 3456), BF16),
        ((ROWS, 3456), BF16),
        ((7, HIST), F32),
    ]
    dma = pltpu.SemaphoreType.DMA
    results = pl.pallas_call(
        kernel,
        out_shape=[pltpu.VMEM(s, t) for s, t in out],
        in_specs=[hbm] * 9 + [pl.BlockSpec(memory_space=pltpu.SMEM)] + [hbm] * 4,
        out_specs=[vmem] * 9,
        scratch_shapes=[
            pltpu.VMEM((SLIM, D), BF16),
            pltpu.VMEM((TINY, D), BF16),
            pltpu.VMEM((TINY, D), BF16),
            pltpu.VMEM((SLIM, D), BF16),
            pltpu.VMEM((WIDE, D), BF16),
            pltpu.VMEM((WIDE, D), BF16),
            pltpu.VMEM((WIDE, D), BF16),
            pltpu.VMEM((2, CACHE, HEAD_DIM), BF16),
            pltpu.VMEM((2, CACHE, HEAD_DIM), BF16),
            pltpu.VMEM((64, ROWS), BF16),
            pltpu.VMEM((7, HIST), F32),
            pltpu.VMEM((1, LANES), F32),
            pltpu.SMEM((2,), jnp.int32),
            pltpu.VMEM((3, D, LANES), BF16),
            pltpu.VMEM((3, N, ROWS, LANES), BF16),
            pltpu.VMEM((8, LANES), F32),
            pltpu.VMEM((1, LANES), F32),
            pltpu.VMEM((N, 1, LANES), F32),
            pltpu.VMEM((1, LANES), F32),
            pltpu.VMEM((TP, 1, LANES), F32),
            pltpu.VMEM((64, 896), F32),
            pltpu.VMEM((4, 16, 896), F32),
            pltpu.VMEM((8, 2, 896), F32),
            pltpu.VMEM((8, 2, 896), F32),
            dma((13,)),
            dma((3, N)),
            dma((3, N)),
            dma((N,)),
            dma((N,)),
            dma((TP,)),
            dma((TP,)),
            dma((4,)),
            dma((4,)),
            dma((8,)),
            dma((8,)),
            pltpu.SemaphoreType.REGULAR((2,)),
            pltpu.VMEM((N, 1, LANES), F32),
            pltpu.VMEM((N, 1, LANES), F32),
            dma((N,)),
            dma((N,)),
        ],
        compiler_params=pltpu.CompilerParams(
            collective_id=0, has_side_effects=True, vmem_limit_bytes=VMEM_LIMIT
        ),
    )(
        *(
            x if x is slot else pltpu.with_memory_space_constraint(x, pltpu.HBM)
            for x in (
                hidden, query_weight.T, key_weight.T, value_weight.T, output_weight, gate_weight.T, up_weight.T,
                down_weight, history, slot, lengths, key_cache, value_cache, spread,
            )
        )
    )
    results = pl.pallas_call(
        finish,
        out_shape=[jax.ShapeDtypeStruct(s, t) for s, t in out],
        in_specs=[vmem] * 9,
        out_specs=[hbm] * 9,
        scratch_shapes=[dma((9,))],
        compiler_params=pltpu.CompilerParams(vmem_limit_bytes=8 * 2**20),
    )(*results)
    attention_out, query, key, value, output, gate, up, down, new_history = results
    return attention_out, query, key, value, output.T, gate, up, down.T, new_history


def solution(mesh):
    f, t = "fsdp", "tp"
    in_specs = (
        P(None, f), P(None, (t, f)), P(None, (t, f)), P(None, (t, f)), P((t, f), None), P(None, (t, f)),
        P(None, (t, f)), P((t, f), None), P(), P(), P(f), P(f, None, t), P(f, None, t),
    )
    out_specs = (P(f, t), P(f, t), P(f, t), P(f, t), P(t, f), P(f, t), P(f, t), P(t, f), P())
    return jax.shard_map(per_device, mesh=mesh, in_specs=in_specs, out_specs=out_specs, check_vma=False)
```
